32 devices in a mesh: sy: 8 (over y, x, core), sx: 4 (over z).
Axes of the slice: x: 2, y: 2, z: 4, core: 2. Of those that a mesh axis runs over, the one named last changes fastest.
Arguments:
- spectrum: bfloat16 [2, 9216, 9216], P(None, 'sy', 'sx'), may hold values from -6 to 6
- pupils: bfloat16 [2, 2048, 2048], P(None, 'sy', 'sx'), may hold values from -6 to 6
- amplitudes: float32 [8, 8, 4, 256, 256], P('sy', 'sx'), may hold values from 0.2 to 2
- crop_starts: int32 [8, 8, 4, 2], P('sy', 'sx'), may hold values from 0 to 896
- led_counts: int32 [8, 8], P('sy', 'sx'), may hold values from 1 to 4, as said below
Outputs:
- spectrum_grad: bfloat16 [2, 9216, 9216], P(None, 'sy', 'sx')
- pupil_grad: float32 [2, 2048, 2048], P(None, 'sy', 'sx')
The draws below stay inside these ranges and needn't reach their ends.
Inputs may be any that keep to these rules, and one draw needn't show every extreme that they name: `led_counts`: slots at or past a segment's count are ignored.
All inputs are finite; a program needn't handle non-finite values.
Results may differ from the reference program's by a relative error of at most 0.001.
Values may be sent and summed in bfloat16 or wider, within the bound.
A program may use at most 256 MiB of HBM per device.

```python
import math
import jax
import jax.numpy as jnp
from jax import lax

W = 256
H = 64
SEG = 1024
MAXL = 4
E = 1152
GY = 8
GX = 8


def draw_crop_starts(key, part):
    subkeys = jax.random.split(key, 2)
    farthest = E - W
    entries = GY * GX * MAXL * 2
    starts = jax.random.randint(subkeys[0], (entries,), 0, farthest + 1)
    chosen = jax.random.permutation(subkeys[1], entries)
    starts = starts.at[chosen[0]].set(0).at[chosen[1]].set(farthest)
    return starts.reshape(GY, GX, MAXL, 2).astype(jnp.int32)


def draw_led_counts(key, part):
    subkeys = jax.random.split(key, 5)
    first_draw = jax.random.randint(subkeys[0], (GY, GX), 1, MAXL + 1)
    second_draw = jax.random.randint(subkeys[1], (GY, GX), 1, MAXL + 1)
    third_draw = jax.random.randint(subkeys[2], (GY, GX), 1, MAXL + 1)
    fewest = jnp.minimum(jnp.minimum(first_draw, second_draw), third_draw)
    pick_row = jax.random.randint(subkeys[3], (), 0, GY)
    pick_col = jax.random.randint(subkeys[4], (), 0, GX // 2) * 2
    fewest = fewest.at[pick_row, pick_col].set(MAXL).at[pick_row, pick_col + 1].set(MAXL)
    return fewest.astype(jnp.int32)


def shard_levels(stream_key, dims, shards, least, top_value):
    def one(dim, parts):
        draws = jax.random.uniform(jax.random.fold_in(jax.random.fold_in(stream_key, 6), dim), (parts,), jnp.float32, least / len(shards), top_value / len(shards))
        return jnp.repeat(jnp.exp(draws), dims[dim] // parts).reshape((-1,) + (1,) * (len(dims) - dim - 1))

    loudness = one(*shards[0])
    for cut in shards[1:]:
        loudness = loudness * one(*cut)
    return loudness


def noise(stream_key, extent, spread, reach, shards=(), kind=jnp.bfloat16):
    level = shard_levels(stream_key, extent, shards, -0.22, 0.18) if shards else 1.0
    values = jax.random.normal(stream_key, extent, jnp.float32) * spread * level
    return jnp.minimum(jnp.maximum(values, -reach), reach).astype(kind)


def setup_inputs(seed: int = 0) -> dict:
    keys = jax.random.split(jax.random.key(seed), 6)
    spectrum = noise(keys[0], (2, GY * E, GX * E), 1.0, 6.0, ((1, 8), (2, 4)))
    pupils = noise(keys[1], (2, GY * W, GX * W), 1.0, 6.0, ((1, 8), (2, 4)))
    amplitudes = jnp.clip(0.2 + 1.8 * jax.random.uniform(keys[2], (GY, GX, MAXL, W, W), jnp.float32) ** shard_levels(keys[2], (GY, GX, MAXL, W, W), ((0, 8), (1, 4)), -0.2, 0.2), 0.2, 2.0)
    crop_starts = draw_crop_starts(jax.random.fold_in(keys[5], 71), 0)
    led_counts = draw_led_counts(jax.random.fold_in(keys[5], 71), 0)
    return dict(spectrum=spectrum, pupils=pupils, amplitudes=amplitudes, crop_starts=crop_starts, led_counts=led_counts)


FLOOR_SQUARE = 0.0625
MU_WEIGHT = 0.5
LAM_WEIGHT = 0.5

def product(first_op, second_op):
    return jnp.dot(first_op, second_op, precision=lax.Precision.HIGHEST, preferred_element_type=jnp.float32)

def dft_tables(side_len):
    positions = jnp.arange(side_len, dtype=jnp.int32)
    phase_index = positions[:, None] * positions[None, :] % side_len
    angles = phase_index.astype(jnp.float32) * (2.0 * math.pi / side_len)
    norm_scale = 1.0 / math.sqrt(side_len)
    return (jnp.cos(angles) * norm_scale, jnp.sin(angles) * norm_scale)

def transform(field_re, field_im, cos_table, sin_table, sign_flip):
    left_re = product(cos_table, field_re) - sign_flip * product(sin_table, field_im)
    left_im = product(cos_table, field_im) + sign_flip * product(sin_table, field_re)
    out_re = product(left_re, cos_table) - sign_flip * product(left_im, sin_table)
    out_im = product(left_im, cos_table) + sign_flip * product(left_re, sin_table)
    return (out_re, out_im)

def segment_data(tile_obj, tile_pup, amp_stack, start_stack, live_count, cos_table, sin_table):
    side_len = tile_pup.shape[1]
    pup_re = tile_pup[0]
    pup_im = tile_pup[1]

    def led_step(slot_index, carried):
        grad_re, grad_im, pgrad_re, pgrad_im = carried
        row_start = start_stack[slot_index, 0]
        col_start = start_stack[slot_index, 1]
        crop_re = lax.dynamic_slice(tile_obj[0], (row_start, col_start), (side_len, side_len))
        crop_im = lax.dynamic_slice(tile_obj[1], (row_start, col_start), (side_len, side_len))
        amp_tile = lax.dynamic_index_in_dim(amp_stack, slot_index, 0, keepdims=False)
        field_re = pup_re * crop_re - pup_im * crop_im
        field_im = pup_re * crop_im + pup_im * crop_re
        psi_re, psi_im = transform(field_re, field_im, cos_table, sin_table, 1.0)
        power_sq = psi_re * psi_re + psi_im * psi_im
        keeper = 1.0 - amp_tile / jnp.sqrt(jnp.maximum(power_sq, FLOOR_SQUARE))
        back_re, back_im = transform(psi_re * keeper, psi_im * keeper, cos_table, sin_table, -1.0)
        dcrop_re = pup_re * back_re + pup_im * back_im
        dcrop_im = pup_re * back_im - pup_im * back_re
        old_re = lax.dynamic_slice(grad_re, (row_start, col_start), (side_len, side_len))
        old_im = lax.dynamic_slice(grad_im, (row_start, col_start), (side_len, side_len))
        grad_re = lax.dynamic_update_slice(grad_re, old_re + dcrop_re, (row_start, col_start))
        grad_im = lax.dynamic_update_slice(grad_im, old_im + dcrop_im, (row_start, col_start))
        pgrad_re = pgrad_re + crop_re * back_re + crop_im * back_im
        pgrad_im = pgrad_im + crop_re * back_im - crop_im * back_re
        return (grad_re, grad_im, pgrad_re, pgrad_im)
    zero_obj = jnp.zeros(tile_obj.shape[1:], jnp.float32)
    zero_pup = jnp.zeros((side_len, side_len), jnp.float32)
    grad_re, grad_im, pgrad_re, pgrad_im = lax.fori_loop(0, live_count, led_step, (zero_obj, zero_obj, zero_pup, zero_pup))
    return (jnp.stack([grad_re, grad_im]), jnp.stack([pgrad_re, pgrad_im]))

def band_range(offset, tile_edge, band_width):
    if offset == 0:
        return (0, 0, tile_edge)
    if offset == 1:
        return (tile_edge - band_width, 0, band_width)
    return (0, tile_edge - band_width, band_width)

def inside(value, limit):
    return jnp.where((value >= 0) & (value < limit), jnp.float32(1.0), jnp.float32(0.0))

def to_tiles(array, grid_rows, grid_cols, tile_edge):
    shaped = array.reshape(2, grid_rows, tile_edge, grid_cols, tile_edge)
    return shaped.transpose(1, 3, 0, 2, 4).reshape(grid_rows * grid_cols, 2, tile_edge, tile_edge)

def from_tiles(tiles, grid_rows, grid_cols, tile_edge):
    shaped = tiles.reshape(grid_rows, grid_cols, 2, tile_edge, tile_edge)
    return shaped.transpose(2, 0, 3, 1, 4).reshape(2, grid_rows * tile_edge, grid_cols * tile_edge)

def reference(spectrum, pupils, amplitudes, crop_starts, led_counts):
    tile_edge = SEG + 2 * H
    band_width = 2 * H
    obj_tiles = to_tiles(spectrum, GY, GX, tile_edge)
    pup_tiles = to_tiles(pupils, GY, GX, W)
    amp_tiles = amplitudes.reshape(GY * GX, MAXL, W, W)
    start_tiles = crop_starts.reshape(GY * GX, MAXL, 2)
    count_tiles = led_counts.reshape(GY * GX)
    cos_table, sin_table = dft_tables(W)

    def one_segment(seg_index):
        seg_row = seg_index // GX
        seg_col = seg_index % GX
        tile_obj = obj_tiles[seg_index].astype(jnp.float32)
        tile_pup = pup_tiles[seg_index].astype(jnp.float32)
        data_obj, data_pup = segment_data(tile_obj, tile_pup, amp_tiles[seg_index], start_tiles[seg_index], count_tiles[seg_index], cos_table, sin_table)
        consist = jnp.zeros_like(tile_obj)
        smooth = jnp.zeros_like(tile_pup)
        for delta_y in (-1, 0, 1):
            for delta_x in (-1, 0, 1):
                if delta_y != 0 or delta_x != 0:
                    near_row = seg_row + delta_y
                    near_col = seg_col + delta_x
                    weight = inside(near_row, GY) * inside(near_col, GX)
                    near_index = jnp.clip(near_row, 0, GY - 1) * GX + jnp.clip(near_col, 0, GX - 1)
                    mine_y, other_y, span_y = band_range(delta_y, tile_edge, band_width)
                    mine_x, other_x, span_x = band_range(delta_x, tile_edge, band_width)
                    neighbour = obj_tiles[near_index][:, other_y:other_y + span_y, other_x:other_x + span_x].astype(jnp.float32)
                    own_band = tile_obj[:, mine_y:mine_y + span_y, mine_x:mine_x + span_x]
                    consist = consist.at[:, mine_y:mine_y + span_y, mine_x:mine_x + span_x].add(weight * (own_band - neighbour))
                    if delta_y == 0 or delta_x == 0:
                        smooth = smooth + weight * (tile_pup - pup_tiles[near_index].astype(jnp.float32))
        grad_obj = (data_obj + MU_WEIGHT * consist).astype(jnp.bfloat16)
        grad_pup = data_pup + LAM_WEIGHT * smooth
        return (grad_obj, grad_pup)
    obj_out, pup_out = lax.map(one_segment, jnp.arange(GY * GX, dtype=jnp.int32))
    return (from_tiles(obj_out, GY, GX, tile_edge), from_tiles(pup_out, GY, GX, W))
```

```python
import functools
import math

import jax
import jax.numpy as jnp
import numpy as np
from jax import lax
from jax.experimental import pallas as pl
from jax.experimental.pallas import tpu as pltpu
from jax.sharding import PartitionSpec as P

H = 64
MAXL = 4
LANES = 128
SUB = 16
FLOOR_SQUARE = 0.0625
MU_WEIGHT = 0.5
LAM_WEIGHT = 0.5
F32 = jnp.float32
BF16 = jnp.bfloat16


def half_tables(side):
    half = side // 2
    n = np.arange(half)[:, None]
    k = np.arange(half)[None, :]
    mats = []
    for odd in (0, 1):
        ang = 2.0 * math.pi * ((n * (2 * k + odd)) % side) / side
        re, im = np.cos(ang) / math.sqrt(side), np.sin(ang) / math.sqrt(side)
        right = np.block([[re, im], [-im, re]])
        mats += [right, right.T]
    mats = np.stack(mats).astype(np.float32)
    hi = mats.astype(jnp.bfloat16)
    lo = (mats - hi.astype(np.float32)).astype(jnp.bfloat16)
    perm = np.zeros((side, side), np.float32)
    perm[2 * np.arange(half), np.arange(half)] = 1.0
    perm[2 * np.arange(half) + 1, half + np.arange(half)] = 1.0
    return np.concatenate([hi, lo, perm.astype(jnp.bfloat16)[None]])


def split(value):
    hi = value.astype(BF16)
    return hi, (value - hi.astype(F32)).astype(BF16)


def dot(a, b):
    return jnp.dot(a, b, preferred_element_type=F32)


def data_kernel(
    start_ref, count_ref, flag_ref, spec, pup, amps, tab,
    out, top_out, bot_out, left_out, right_out, pgrad,
    acc, stage, win, ampbuf, wf, crop, xs, ys, ampp, rows_buf, sides,
    in_sem, band_sem, out_sem,
):
    cols_dev = amps.shape[0]
    pw = pup.shape[1]
    half = pw // 2
    edge = spec.shape[1]
    band = 2 * H
    win_r, win_c = win.shape[2], win.shape[3]
    mid = edge - 2 * band
    CH = 32
    last = edge // LANES - 1
    win_t = win_c // LANES

    def where_of(seg, slot):
        base = (seg * MAXL + slot) * 2
        a = start_ref[base]
        b = start_ref[base + 1]
        a_al = jnp.minimum(a // SUB * SUB, edge - win_r)
        b_al = jnp.minimum(b // LANES * LANES, edge - win_c)
        return a, b, a_al, b_al

    def fetch(seg, slot, buf):
        a, b, a_al, b_al = where_of(seg, slot)
        rs = pl.multiple_of(a_al, SUB)
        cs = pl.multiple_of(seg * edge + b_al, LANES)
        return (
            pltpu.make_async_copy(
                spec.at[:, pl.ds(rs, win_r), pl.ds(cs, win_c)], win.at[buf], in_sem.at[0, buf]
            ),
        ) + tuple(
            pltpu.make_async_copy(
                amps.at[seg, slot, :, t * LANES : (t + 1) * LANES],
                ampbuf.at[buf, t],
                in_sem.at[1 + t, buf],
            )
            for t in range(pw // LANES)
        )

    for c in fetch(0, 0, 0):
        c.start()
    loads = [
        pltpu.make_async_copy(spec.at[:, 0:band, :], rows_buf.at[0], band_sem.at[0]),
        pltpu.make_async_copy(spec.at[:, edge - band :, :], rows_buf.at[1], band_sem.at[1]),
    ]
    for s in range(cols_dev):
        for j, c0 in enumerate((s * edge, (s + 1) * edge - band)):
            loads.append(
                pltpu.make_async_copy(
                    spec.at[:, :, c0 : c0 + band], sides.at[2 * s + j], band_sem.at[2 + 2 * s + j]
                )
            )
    for c in loads:
        c.start()
    w_top, w_bot, w_left, w_right = (flag_ref[i] for i in range(4))

    def zero_acc(seg):
        def zero(i, _):
            r = pl.multiple_of(i * 8, 8)
            for p in range(2):
                for t in range(edge // LANES):
                    acc[seg, p, t, pl.ds(r, 8), :] = jnp.zeros((8, LANES), F32)
            return 0

        lax.fori_loop(0, edge // 8, zero, 0)
        for p in range(2):
            pgrad[p, :, pl.ds(pl.multiple_of(seg * pw, LANES), pw)] = jnp.zeros((pw, pw), F32)

    def own_terms(seg):
        wl = jnp.where(seg == 0, w_left, 1.0)
        wr = jnp.where(seg == cols_dev - 1, w_right, 1.0)
        il = jnp.where(seg == 0, 0.0, 1.0)
        ir = jnp.where(seg == cols_dev - 1, 0.0, 1.0)
        lo_nb = jnp.maximum(2 * seg - 1, 0)
        hi_nb = jnp.minimum(2 * seg + 2, 2 * cols_dev - 1)
        cbase = pl.multiple_of(seg * edge, LANES)

        def side(i, _):
            r = pl.multiple_of(i * SUB, SUB)
            vert = 1.0 + jnp.where(r < band, w_top, 0.0) + jnp.where(r >= edge - band, w_bot, 0.0)
            for p in range(2):
                mine = sides[2 * seg, p, pl.ds(r, SUB), :].astype(F32)
                other = sides[lo_nb, p, pl.ds(r, SUB), :].astype(F32)
                acc[seg, p, 0, pl.ds(r, SUB), :] += MU_WEIGHT * (wl * vert * mine - il * other)
                mine = sides[2 * seg + 1, p, pl.ds(r, SUB), :].astype(F32)
                other = sides[hi_nb, p, pl.ds(r, SUB), :].astype(F32)
                acc[seg, p, last, pl.ds(r, SUB), :] += MU_WEIGHT * (
                    wr * vert * mine - ir * other
                )
            return 0

        lax.fori_loop(0, edge // SUB, side, 0)

        def flat(i, _):
            r = pl.multiple_of(i * SUB, SUB)
            for p in range(2):
                for j, w in ((0, w_top), (1, w_bot)):
                    mine = rows_buf[j, p, pl.ds(r, SUB), pl.ds(cbase, edge)].astype(F32)
                    rs = pl.ds(pl.multiple_of(r + j * (edge - band), SUB), SUB)
                    for t in range(edge // LANES):
                        acc[seg, p, t, rs, :] += (MU_WEIGHT * w) * mine[
                            :, t * LANES : (t + 1) * LANES
                        ]
            return 0

        lax.fori_loop(0, band // SUB, flat, 0)
        pc = pl.multiple_of(seg * pw, LANES)
        pl_c = pl.multiple_of(jnp.maximum(seg - 1, 0) * pw, LANES)
        pr_c = pl.multiple_of(jnp.minimum(seg + 1, cols_dev - 1) * pw, LANES)
        near = w_top + w_bot + wl + wr

        def pups(i, _):
            r = pl.multiple_of(i * SUB, SUB)
            for p in range(2):
                mine = pup[p, pl.ds(r, SUB), pl.ds(pc, pw)].astype(F32)
                lef = pup[p, pl.ds(r, SUB), pl.ds(pl_c, pw)].astype(F32)
                rig = pup[p, pl.ds(r, SUB), pl.ds(pr_c, pw)].astype(F32)
                pgrad[p, pl.ds(r, SUB), pl.ds(pc, pw)] += LAM_WEIGHT * (
                    near * mine - il * lef - ir * rig
                )
            return 0

        lax.fori_loop(0, pw // SUB, pups, 0)

    def put(which, rows, cols, value):
        hi, lo = split(value)
        xs[which, 0, rows, cols] = hi
        xs[which, 1, rows, cols] = lo

    def from_right(which, table):
        lhs = jnp.concatenate([xs[which, 0], xs[which, 1], xs[which, 0]], axis=1)
        rhs = jnp.concatenate([tab[table], tab[table], tab[4 + table]], axis=0)
        ys[which] = dot(lhs, rhs)

    def from_left(which, table):
        rhs = jnp.concatenate([xs[which, 0], xs[which, 1], xs[which, 0]], axis=0)
        lhs = jnp.concatenate([tab[table], tab[table], tab[4 + table]], axis=1)
        ys[which] = dot(lhs, rhs)

    lo_c, hi_c, all_c = slice(0, half), slice(half, pw), slice(0, pw)

    def slot_step(seg, slot, count):
        buf = lax.rem(count, 2)
        more = slot + 1 < count_ref[seg]
        nseg = jnp.where(more, seg, seg + 1)
        nslot = jnp.where(more, slot + 1, 0)

        @pl.when(nseg < cols_dev)
        def _():
            for c in fetch(nseg, nslot, 1 - buf):
                c.start()

        for c in fetch(seg, slot, buf):
            c.wait()
        a, b, a_al, b_al = where_of(seg, slot)
        a_off = a - a_al
        b_off = b - b_al
        pc = pl.multiple_of(seg * pw, LANES)
        for p in range(2):
            for r in range(0, win_r, SUB):
                wide = win[buf, p, r : r + SUB, :].astype(F32)
                for t in range(win_t):
                    wf[p, t, r : r + SUB, :] = wide[:, t * LANES : (t + 1) * LANES]
        back_roll = lax.rem(win_c - b_off, win_c)
        for r in range(0, pw, CH):
            rows = slice(r, r + CH)
            cre, cim = (
                pltpu.roll(
                    jnp.concatenate(
                        [wf[p, t, pl.ds(a_off + r, CH), :] for t in range(win_t)], axis=1
                    ),
                    back_roll,
                    axis=1,
                )[:, :pw]
                for p in range(2)
            )
            crop[0, rows, :] = cre
            crop[1, rows, :] = cim
            pre = pup[0, rows, pl.ds(pc, pw)].astype(F32)
            pim = pup[1, rows, pl.ds(pc, pw)].astype(F32)
            fre = pre * cre - pim * cim
            fim = pre * cim + pim * cre
            put(0, rows, lo_c, fre[:, lo_c] + fre[:, hi_c])
            put(0, rows, hi_c, fim[:, lo_c] + fim[:, hi_c])
            put(1, rows, lo_c, fre[:, lo_c] - fre[:, hi_c])
            put(1, rows, hi_c, fim[:, lo_c] - fim[:, hi_c])
        from_right(0, 0)
        from_right(1, 2)
        for r in range(0, half, CH):
            for part, cols in ((0, lo_c), (1, hi_c)):
                rows = slice(part * half + r, part * half + r + CH)
                for which, ocols in ((0, lo_c), (1, hi_c)):
                    upper = ys[which, r : r + CH, cols]
                    lower = ys[which, half + r : half + r + CH, cols]
                    put(2, rows, ocols, upper + lower)
                    put(3, rows, ocols, upper - lower)
        ahi, alo = [], []
        for odd in range(2):
            h, l = split(
                jnp.concatenate(
                    [ampbuf[buf, t, pl.ds(odd, half, stride=2), :] for t in range(pw // LANES)],
                    axis=1,
                )
            )
            ahi.append(h)
            alo.append(l)
        lhs = jnp.concatenate(
            [jnp.concatenate(ahi, axis=0), jnp.concatenate(alo, axis=0)], axis=1
        )
        ampp[...] = dot(lhs, jnp.concatenate([tab[8], tab[8]], axis=0))
        from_left(2, 1)
        from_left(3, 3)
        for which in range(2):
            for r in range(0, half, CH):
                re = ys[2 + which, r : r + CH, :]
                im = ys[2 + which, half + r : half + r + CH, :]
                amp = ampp[which * half + r : which * half + r + CH, :]
                keep = 1.0 - amp * lax.rsqrt(jnp.maximum(re * re + im * im, FLOOR_SQUARE))
                put(which, slice(r, r + CH), all_c, re * keep)
                put(which, slice(half + r, half + r + CH), all_c, im * keep)
        from_left(0, 0)
        from_left(1, 2)
        for r in range(0, half, CH):
            for part, cols in ((0, lo_c), (1, hi_c)):
                even = ys[0, part * half + r : part * half + r + CH, :]
                odd = ys[1, part * half + r : part * half + r + CH, :]
                upper, lower = even + odd, even - odd
                for rows, val in (
                    (slice(r, r + CH), upper), (slice(half + r, half + r + CH), lower),
                ):
                    put(2, rows, cols, val[:, lo_c])
                    put(3, rows, cols, val[:, hi_c])
        from_right(2, 1)
        from_right(3, 3)
        tile0 = b_al // LANES
        for r in range(0, pw, CH):
            rows = slice(r, r + CH)
            even, odd = ys[2, rows, :], ys[3, rows, :]
            plus, minus = even + odd, even - odd
            bre = jnp.concatenate([plus[:, lo_c], minus[:, lo_c]], axis=1)
            bim = jnp.concatenate([plus[:, hi_c], minus[:, hi_c]], axis=1)
            pre = pup[0, rows, pl.ds(pc, pw)].astype(F32)
            pim = pup[1, rows, pl.ds(pc, pw)].astype(F32)
            cre, cim = crop[0, rows, :], crop[1, rows, :]
            pgrad[0, rows, pl.ds(pc, pw)] += cre * bre + cim * bim
            pgrad[1, rows, pl.ds(pc, pw)] += cre * bim - cim * bre
            blank = jnp.zeros((CH, win_c - pw), F32)
            for p, val in ((0, pre * bre + pim * bim), (1, pre * bim - pim * bre)):
                wide = pltpu.roll(jnp.concatenate([val, blank], axis=1), b_off, axis=1)
                for t in range(win_t):
                    acc[seg, p, tile0 + t, pl.ds(a + r, CH), :] += wide[
                        :, t * LANES : (t + 1) * LANES
                    ]
        return count + 1

    def outs(seg):
        cb = pl.multiple_of(seg * edge, LANES)
        return [
            pltpu.make_async_copy(
                stage.at[seg], out.at[:, band : band + mid, pl.ds(cb, edge)], out_sem.at[0, seg]
            ),
            pltpu.make_async_copy(
                acc.at[seg, :, :, 0:band, :], top_out.at[:, seg], out_sem.at[1, seg]
            ),
            pltpu.make_async_copy(
                acc.at[seg, :, :, edge - band :, :], bot_out.at[:, seg], out_sem.at[2, seg]
            ),
        ]

    left_copy = pltpu.make_async_copy(
        acc.at[0, :, 0, band : band + mid, :], left_out, out_sem.at[3, 0]
    )
    right_copy = pltpu.make_async_copy(
        acc.at[cols_dev - 1, :, last, band : band + mid, :], right_out, out_sem.at[3, 1]
    )

    def segment(seg, count):
        zero_acc(seg)

        @pl.when(seg == 0)
        def _():
            for c in loads:
                c.wait()

        own_terms(seg)
        count = lax.fori_loop(
            0, count_ref[seg], lambda slot, c: slot_step(seg, slot, c), count
        )

        def conv(i, _):
            r = pl.multiple_of(i * SUB, SUB)
            for p in range(2):
                rs = pl.ds(pl.multiple_of(r + band, SUB), SUB)
                for t in range(edge // LANES):
                    stage[seg, p, pl.ds(r, SUB), t * LANES : (t + 1) * LANES] = acc[
                        seg, p, t, rs, :
                    ].astype(BF16)
            return 0

        lax.fori_loop(0, mid // SUB, conv, 0)
        for c in outs(seg):
            c.start()
        return count

    lax.fori_loop(0, cols_dev, segment, jnp.int32(0))
    left_copy.start()
    right_copy.start()
    for s in range(cols_dev):
        for c in outs(s):
            c.wait()
    left_copy.wait()
    right_copy.wait()


def patch_kernel(
    base, top, bot, left, right, pgrad, up, down, west, east, nw, ne, sw, se,
    out, pout, tb, bb, lb, rb, sem,
):
    edge = base.shape[1]
    width = base.shape[2]
    band = 2 * H
    mid = edge - 2 * band
    cols_dev = width // edge
    pw = pgrad.shape[1]
    half_w = MU_WEIGHT

    def rows_work(i, _):
        r = pl.multiple_of(i * SUB, SUB)
        rs = pl.ds(r, SUB)
        for p in range(2):
            for acc, halo, buf, wc, ec, side0 in (
                (top, up, tb, nw, ne, 0), (bot, down, bb, sw, se, edge - band),
            ):
                srs = pl.ds(pl.multiple_of(r + side0, SUB), SUB)
                for s in range(cols_dev):
                    for t in range(edge // LANES):
                        c0 = s * edge + t * LANES
                        total = halo[p, rs, c0 : c0 + LANES].astype(F32)
                        if t == 0 or t == edge // LANES - 1:
                            o0 = c0 + LANES if t else c0 - LANES
                            if 0 <= o0 < width:
                                total = total + halo[p, rs, o0 : o0 + LANES].astype(F32)
                            elif t:
                                total = total + ec[p, rs, :].astype(F32)
                                total = total + east[p, srs, :].astype(F32)
                            else:
                                total = total + wc[p, rs, :].astype(F32)
                                total = total + west[p, srs, :].astype(F32)
                        buf[p, rs, c0 : c0 + LANES] = (
                            acc[p, s, t, rs, :] - half_w * total
                        ).astype(BF16)
        return 0

    lax.fori_loop(0, band // SUB, rows_work, 0)
    copies = [
        pltpu.make_async_copy(tb, out.at[:, 0:band, :], sem.at[0]),
        pltpu.make_async_copy(bb, out.at[:, edge - band :, :], sem.at[1]),
    ]
    for c in copies:
        c.start()

    def mid_work(i, _):
        rs = pl.ds(pl.multiple_of(i * SUB, SUB), SUB)
        srs = pl.ds(pl.multiple_of(i * SUB + band, SUB), SUB)
        for p in range(2):
            lb[p, rs, :] = (left[p, rs, :] - half_w * west[p, srs, :].astype(F32)).astype(BF16)
            rb[p, rs, :] = (right[p, rs, :] - half_w * east[p, srs, :].astype(F32)).astype(BF16)
        return 0

    lax.fori_loop(0, mid // SUB, mid_work, 0)
    more = [
        pltpu.make_async_copy(lb, out.at[:, band : band + mid, 0:band], sem.at[2]),
        pltpu.make_async_copy(rb, out.at[:, band : band + mid, width - band :], sem.at[3]),
    ]
    for c in more:
        c.start()
    pwide = cols_dev * pw
    for piece in range(pw // band):
        for r in range(0, band, SUB):
            rows = slice(piece * band + r, piece * band + r + SUB)
            vs = slice(width + piece * pwide, width + (piece + 1) * pwide)
            for p in range(2):
                near = up[p, r : r + SUB, vs].astype(F32) + down[p, r : r + SUB, vs].astype(F32)
                pout[p, rows, :] = pgrad[p, rows, :] - LAM_WEIGHT * near
    for piece in range(pw // LANES):
        for r in range(0, pw, SUB):
            rows = slice(r, r + SUB)
            hs = slice(edge + piece * pw + r, edge + piece * pw + r + SUB)
            for p in range(2):
                wc = slice(piece * LANES, (piece + 1) * LANES)
                ec = slice(pwide - pw + piece * LANES, pwide - pw + (piece + 1) * LANES)
                pout[p, rows, wc] -= LAM_WEIGHT * west[p, hs, :].astype(F32)
                pout[p, rows, ec] -= LAM_WEIGHT * east[p, hs, :].astype(F32)
    for c in copies + more:
        c.wait()


def shift(block, axes, step):
    sizes = [lax.axis_size(a) for a in axes]
    pairs = []
    for i in range(math.prod(sizes)):
        at = np.unravel_index(i, sizes)
        to = [int(x) + d for x, d in zip(at, step)]
        if all(0 <= x < n for x, n in zip(to, sizes)):
            pairs.append((i, int(np.ravel_multi_index(to, sizes))))
    return lax.ppermute(block, axes if len(axes) > 1 else axes[0], pairs)


def local(spectrum, pupils, amplitudes, crop_starts, led_counts):
    cols_dev = amplitudes.shape[1]
    pw = pupils.shape[1]
    edge = spectrum.shape[1]
    width = spectrum.shape[2]
    band = 2 * H
    mid = edge - 2 * band

    def vert(rows):
        pieces = [pupils[:, r : r + band, :] for r in range(0, pw, band)]
        return jnp.concatenate([rows] + pieces, axis=2)

    def horiz(cols, seg):
        pieces = [
            pupils[:, :, seg * pw + c : seg * pw + c + LANES] for c in range(0, pw, LANES)
        ]
        return jnp.concatenate([cols] + pieces, axis=1)

    tops, bots = spectrum[:, :band, :], spectrum[:, edge - band :, :]
    west = shift(horiz(spectrum[:, :, width - band :], cols_dev - 1), ("sx",), (1,))
    east = shift(horiz(spectrum[:, :, :band], 0), ("sx",), (-1,))
    up = shift(vert(bots), ("sy",), (1,))
    down = shift(vert(tops), ("sy",), (-1,))
    both = ("sy", "sx")
    nw = shift(bots[:, :, width - band :], both, (1, 1))
    ne = shift(bots[:, :, :band], both, (1, -1))
    sw = shift(tops[:, :, width - band :], both, (-1, 1))
    se = shift(tops[:, :, :band], both, (-1, -1))

    iy, ix = lax.axis_index("sy"), lax.axis_index("sx")
    flags = jnp.stack(
        [iy > 0, iy < lax.axis_size("sy") - 1, ix > 0, ix < lax.axis_size("sx") - 1]
    ).astype(F32)
    table = jnp.asarray(half_tables(pw))
    smem = pl.BlockSpec(memory_space=pltpu.SMEM)
    vmem = pl.BlockSpec(memory_space=pltpu.VMEM)
    hbm = pl.BlockSpec(memory_space=pltpu.HBM)
    win_r, win_c = pw + SUB, pw + LANES
    base, top, bot, left, right, pgrad = pl.pallas_call(
        data_kernel,
        out_shape=(
            jax.ShapeDtypeStruct(spectrum.shape, BF16),
            jax.ShapeDtypeStruct((2, cols_dev, edge // LANES, band, LANES), F32),
            jax.ShapeDtypeStruct((2, cols_dev, edge // LANES, band, LANES), F32),
            jax.ShapeDtypeStruct((2, mid, band), F32),
            jax.ShapeDtypeStruct((2, mid, band), F32),
            jax.ShapeDtypeStruct(pupils.shape, F32),
        ),
        in_specs=[smem, smem, smem, hbm, vmem, hbm, vmem],
        out_specs=(hbm, hbm, hbm, hbm, hbm, vmem),
        scratch_shapes=[
            pltpu.VMEM((cols_dev, 2, edge // LANES, edge, LANES), F32),
            pltpu.VMEM((cols_dev, 2, mid, edge), BF16),
            pltpu.VMEM((2, 2, win_r, win_c), BF16),
            pltpu.VMEM((2, pw // LANES, pw, LANES), F32),
            pltpu.VMEM((2, win_c // LANES, win_r, LANES), F32),
            pltpu.VMEM((2, pw, pw), F32),
            pltpu.VMEM((4, 2, pw, pw), BF16),
            pltpu.VMEM((4, pw, pw), F32),
            pltpu.VMEM((pw, pw), F32),
            pltpu.VMEM((2, 2, band, width), BF16),
            pltpu.VMEM((2 * cols_dev, 2, edge, band), BF16),
            pltpu.SemaphoreType.DMA((1 + pw // LANES, 2)),
            pltpu.SemaphoreType.DMA((2 + 2 * cols_dev,)),
            pltpu.SemaphoreType.DMA((4, max(cols_dev, 2))),
        ],
        compiler_params=pltpu.CompilerParams(vmem_limit_bytes=60 * 2**20),
        cost_estimate=pl.CostEstimate(
            flops=20_000_000_000, bytes_accessed=30_000_000, transcendentals=0
        ),
        name="slots",
    )(crop_starts.reshape(-1), led_counts.reshape(-1), flags, spectrum, pupils, amplitudes[0], table)
    return pl.pallas_call(
        patch_kernel,
        out_shape=(
            jax.ShapeDtypeStruct(spectrum.shape, BF16),
            jax.ShapeDtypeStruct(pupils.shape, F32),
        ),
        in_specs=[hbm] + [vmem] * 13,
        out_specs=(hbm, vmem),
        scratch_shapes=[
            pltpu.VMEM((2, band, width), BF16),
            pltpu.VMEM((2, band, width), BF16),
            pltpu.VMEM((2, mid, band), BF16),
            pltpu.VMEM((2, mid, band), BF16),
            pltpu.SemaphoreType.DMA((4,)),
        ],
        input_output_aliases={0: 0},
        compiler_params=pltpu.CompilerParams(vmem_limit_bytes=40 * 2**20),
        name="patch",
    )(base, top, bot, left, right, pgrad, up, down, west, east, nw, ne, sw, se)


def solution(mesh):
    placed = (
        P(None, "sy", "sx"),
        P(None, "sy", "sx"),
        P("sy", "sx", None, None, None),
        P("sy", "sx", None, None),
        P("sy", "sx"),
    )
    return jax.shard_map(
        local,
        mesh=mesh,
        in_specs=placed,
        out_specs=(P(None, "sy", "sx"), P(None, "sy", "sx")),
        check_vma=False,
    )
```

```python
import functools
import math

import jax
import jax.numpy as jnp
import numpy as np
from jax import lax
from jax.experimental import pallas as pl
from jax.experimental.pallas import tpu as pltpu
from jax.sharding import PartitionSpec as P

H = 64
MAXL = 4
LANES = 128
CH = 32
SUB = 16
FLOOR_SQUARE = 0.0625
MU_WEIGHT = 0.5
LAM_WEIGHT = 0.5
F32 = jnp.float32
BF16 = jnp.bfloat16

def half_tables(side):
    half = side // 2
    n = np.arange(half)[:, None]
    k = np.arange(half)[None, :]
    mats = []
    for odd in (0, 1):
        ang = 2.0 * math.pi * ((n * (2 * k + odd)) % side) / side
        re, im = np.cos(ang) / math.sqrt(side), np.sin(ang) / math.sqrt(side)
        right = np.block([[re, im], [-im, re]])
        mats += [right, right.T]
    mats = np.stack(mats).astype(np.float32)
    hi = mats.astype(jnp.bfloat16)
    lo = (mats - hi.astype(np.float32)).astype(jnp.bfloat16)
    perm = np.zeros((side, side), np.float32)
    perm[2 * np.arange(half), np.arange(half)] = 1.0
    perm[2 * np.arange(half) + 1, half + np.arange(half)] = 1.0
    return np.concatenate([hi, lo, perm.astype(jnp.bfloat16)[None]])


def split(value):
    hi = value.astype(BF16)
    return hi, (value - hi.astype(F32)).astype(BF16)


def dot(a, b):
    return jnp.dot(a, b, preferred_element_type=F32)


def window_of(start_ref, seg, slot, edge, win_r, win_c):
    base = (seg * MAXL + slot) * 2
    a = start_ref[base]
    b = start_ref[base + 1]
    a_al = jnp.minimum(a // SUB * SUB, edge - win_r)
    b_al = jnp.minimum(b // LANES * LANES, edge - win_c)
    return a, b, a_al, b_al


def crop_kernel(start_ref, count_ref, spec, crops, win, wf, in_sem):
    pw = crops.shape[2]
    edge = spec.shape[1]
    cols_dev = spec.shape[2] // edge
    win_r, win_c = win.shape[2], win.shape[3]
    win_t = win_c // LANES

    def fetch(seg, slot, buf):
        _, _, a_al, b_al = window_of(start_ref, seg, slot, edge, win_r, win_c)
        rs = pl.multiple_of(a_al, SUB)
        cs = pl.multiple_of(seg * edge + b_al, LANES)
        return pltpu.make_async_copy(
            spec.at[:, pl.ds(rs, win_r), pl.ds(cs, win_c)], win.at[buf], in_sem.at[buf]
        )

    fetch(0, 0, 0).start()

    def slot_step(seg, slot, count):
        buf = lax.rem(count, 2)
        more = slot + 1 < count_ref[seg]
        nseg = jnp.where(more, seg, seg + 1)
        nslot = jnp.where(more, slot + 1, 0)

        @pl.when(nseg < cols_dev)
        def _():
            fetch(nseg, nslot, 1 - buf).start()

        fetch(seg, slot, buf).wait()
        a, b, a_al, b_al = window_of(start_ref, seg, slot, edge, win_r, win_c)
        a_off = a - a_al
        for p in range(2):
            for r in range(0, win_r, SUB):
                wide = win[buf, p, r : r + SUB, :].astype(F32)
                for t in range(win_t):
                    wf[p, t, r : r + SUB, :] = wide[:, t * LANES : (t + 1) * LANES]
        back_roll = lax.rem(win_c - (b - b_al), win_c)
        for r in range(0, pw, CH):
            for p in range(2):
                wide = jnp.concatenate(
                    [wf[p, t, pl.ds(a_off + r, CH), :] for t in range(win_t)], axis=1
                )
                crops[seg * MAXL + slot, p, r : r + CH, :] = pltpu.roll(
                    wide, back_roll, axis=1
                )[:, :pw].astype(BF16)
        return count + 1

    def segment(seg, count):
        return lax.fori_loop(
            0, count_ref[seg], lambda slot, c: slot_step(seg, slot, c), count
        )

    lax.fori_loop(0, cols_dev, segment, jnp.int32(0))


def wave_kernel(
    spec, pup_hbm, amps, crops, pup, tab,
    backs, up, down, west, east, pup_up, pup_down, pup_west, pup_east, nw, ne, sw, se,
    ampbuf, xs, ys, ampp, in_sem, send_sem, recv_sem,
):
    pw = pup.shape[1]
    half = pw // 2
    edge = spec.shape[1]
    width = spec.shape[2]
    pwide = pup.shape[2]
    band = 2 * H
    total = crops.shape[0]
    iy, ix = lax.axis_index("sy"), lax.axis_index("sx")
    ny, nx = lax.axis_size("sy"), lax.axis_size("sx")
    has = {}
    for dy in (-1, 0, 1):
        for dx in (-1, 0, 1):
            ok = (iy + dy >= 0) & (iy + dy < ny) & (ix + dx >= 0) & (ix + dx < nx)
            has[dy, dx] = ok

    barrier = pltpu.get_barrier_semaphore()
    near = [(dy, dx) for dy in (-1, 0, 1) for dx in (-1, 0, 1) if dy or dx]
    for dy, dx in near:
        @pl.when(has[dy, dx])
        def _(dy=dy, dx=dx):
            pl.semaphore_signal(
                barrier, inc=1, device_id=(iy + dy, ix + dx),
                device_id_type=pl.DeviceIdType.MESH,
            )
    pl.semaphore_wait(barrier, sum(has[d].astype(jnp.int32) for d in near))
    tops, bots = slice(0, band), slice(edge - band, edge)
    lefts, rights = slice(0, band), slice(width - band, width)
    moves = [
        ((1, 0), spec.at[:, bots, :], up),
        ((-1, 0), spec.at[:, tops, :], down),
        ((0, 1), spec.at[:, :, rights], west),
        ((0, -1), spec.at[:, :, lefts], east),
        ((1, 0), pup_hbm, pup_up),
        ((-1, 0), pup_hbm, pup_down),
        ((0, 1), pup_hbm.at[:, :, pwide - pw :], pup_west),
        ((0, -1), pup_hbm.at[:, :, :pw], pup_east),
        ((1, 1), spec.at[:, bots, rights], nw),
        ((1, -1), spec.at[:, bots, lefts], ne),
        ((-1, 1), spec.at[:, tops, rights], sw),
        ((-1, -1), spec.at[:, tops, lefts], se),
    ]
    copies = []
    for n, ((dy, dx), src, dst) in enumerate(moves):
        copies.append(
            pltpu.make_async_remote_copy(
                src_ref=src, dst_ref=dst, send_sem=send_sem.at[n], recv_sem=recv_sem.at[n],
                device_id=(iy + dy, ix + dx), device_id_type=pl.DeviceIdType.MESH,
            )
        )
    for c, ((dy, dx), _, _) in zip(copies, moves):
        @pl.when(has[dy, dx])
        def _(c=c):
            c.start()

    def put(which, rows, cols, value):
        hi, lo = split(value)
        xs[which, 0, rows, cols] = hi
        xs[which, 1, rows, cols] = lo

    def from_right(which, table):
        lhs = jnp.concatenate([xs[which, 0], xs[which, 1], xs[which, 0]], axis=1)
        rhs = jnp.concatenate([tab[table], tab[table], tab[4 + table]], axis=0)
        ys[which] = dot(lhs, rhs)

    def from_left(which, table):
        rhs = jnp.concatenate([xs[which, 0], xs[which, 1], xs[which, 0]], axis=0)
        lhs = jnp.concatenate([tab[table], tab[table], tab[4 + table]], axis=1)
        ys[which] = dot(lhs, rhs)

    lo_c, hi_c, all_c = slice(0, half), slice(half, pw), slice(0, pw)

    def fetch(i, buf):
        seg = lax.div(i, MAXL)
        slot = lax.rem(i, MAXL)
        return [
            pltpu.make_async_copy(
                amps.at[seg, slot, :, t * LANES : (t + 1) * LANES],
                ampbuf.at[buf, t],
                in_sem.at[t, buf],
            )
            for t in range(pw // LANES)
        ]

    for c in fetch(0, 0):
        c.start()

    def slot_step(i, _):
        buf = lax.rem(i, 2)

        @pl.when(i + 1 < total)
        def _():
            for c in fetch(i + 1, 1 - buf):
                c.start()

        for c in fetch(i, buf):
            c.wait()
        pc = pl.multiple_of(lax.div(i, MAXL) * pw, LANES)
        for r in range(0, pw, CH):
            rows = slice(r, r + CH)
            cre = crops[i, 0, rows, :].astype(F32)
            cim = crops[i, 1, rows, :].astype(F32)
            pre = pup[0, rows, pl.ds(pc, pw)].astype(F32)
            pim = pup[1, rows, pl.ds(pc, pw)].astype(F32)
            fre = pre * cre - pim * cim
            fim = pre * cim + pim * cre
            put(0, rows, lo_c, fre[:, lo_c] + fre[:, hi_c])
            put(0, rows, hi_c, fim[:, lo_c] + fim[:, hi_c])
            put(1, rows, lo_c, fre[:, lo_c] - fre[:, hi_c])
            put(1, rows, hi_c, fim[:, lo_c] - fim[:, hi_c])
        from_right(0, 0)
        from_right(1, 2)
        for r in range(0, half, CH):
            for part, cols in ((0, lo_c), (1, hi_c)):
                rows = slice(part * half + r, part * half + r + CH)
                for which, ocols in ((0, lo_c), (1, hi_c)):
                    upper = ys[which, r : r + CH, cols]
                    lower = ys[which, half + r : half + r + CH, cols]
                    put(2, rows, ocols, upper + lower)
                    put(3, rows, ocols, upper - lower)
        ahi, alo = [], []
        for odd in range(2):
            h, l = split(
                jnp.concatenate(
                    [ampbuf[buf, t, pl.ds(odd, half, stride=2), :] for t in range(pw // LANES)],
                    axis=1,
                )
            )
            ahi.append(h)
            alo.append(l)
        lhs = jnp.concatenate(
            [jnp.concatenate(ahi, axis=0), jnp.concatenate(alo, axis=0)], axis=1
        )
        ampp[...] = dot(lhs, jnp.concatenate([tab[8], tab[8]], axis=0))
        from_left(2, 1)
        from_left(3, 3)
        for which in range(2):
            for r in range(0, half, CH):
                re = ys[2 + which, r : r + CH, :]
                im = ys[2 + which, half + r : half + r + CH, :]
                amp = ampp[which * half + r : which * half + r + CH, :]
                keep = 1.0 - amp * lax.rsqrt(jnp.maximum(re * re + im * im, FLOOR_SQUARE))
                put(which, slice(r, r + CH), all_c, re * keep)
                put(which, slice(half + r, half + r + CH), all_c, im * keep)
        from_left(0, 0)
        from_left(1, 2)
        for r in range(0, half, CH):
            for part, cols in ((0, lo_c), (1, hi_c)):
                even = ys[0, part * half + r : part * half + r + CH, :]
                odd = ys[1, part * half + r : part * half + r + CH, :]
                upper, lower = even + odd, even - odd
                for rows, val in (
                    (slice(r, r + CH), upper), (slice(half + r, half + r + CH), lower),
                ):
                    put(2, rows, cols, val[:, lo_c])
                    put(3, rows, cols, val[:, hi_c])
        from_right(2, 1)
        from_right(3, 3)
        for r in range(0, pw, CH):
            rows = slice(r, r + CH)
            even, odd = ys[2, rows, :], ys[3, rows, :]
            plus, minus = even + odd, even - odd
            backs[i, 0, rows, lo_c] = plus[:, lo_c]
            backs[i, 0, rows, hi_c] = minus[:, lo_c]
            backs[i, 1, rows, lo_c] = plus[:, hi_c]
            backs[i, 1, rows, hi_c] = minus[:, hi_c]
        return 0

    lax.fori_loop(0, total, slot_step, 0)
    for c, ((dy, dx), _, _) in zip(copies, moves):
        @pl.when(has[dy, dx])
        def _(c=c):
            c.wait_send()

        @pl.when(has[-dy, -dx])
        def _(c=c):
            c.wait_recv()


def finish_kernel(
    start_ref, count_ref, flag_ref, spec, pup, crops, backs,
    up, down, west, east, pup_up, pup_down, pup_west, pup_east, nw, ne, sw, se,
    out, pgrad,
    acc, stage, rows_buf, sides, hrows, hsides, hcorn, hpv, hph, band_sem, out_sem,
):
    pw = pup.shape[1]
    edge = spec.shape[1]
    cols_dev = spec.shape[2] // edge
    band = 2 * H
    win_r, win_c = pw + SUB, pw + LANES
    win_t = win_c // LANES
    last = edge // LANES - 1
    w_top, w_bot, w_left, w_right = (flag_ref[i] for i in range(4))
    loads = [
        (spec.at[:, 0:band, :], rows_buf.at[0]),
        (spec.at[:, edge - band :, :], rows_buf.at[1]),
    ]
    for s in range(cols_dev):
        for j, c0 in enumerate((s * edge, (s + 1) * edge - band)):
            loads.append((spec.at[:, :, c0 : c0 + band], sides.at[2 * s + j]))
    loads += [
        (up, hrows.at[0]), (down, hrows.at[1]), (west, hsides.at[0]), (east, hsides.at[1]),
        (nw, hcorn.at[0]), (ne, hcorn.at[1]), (sw, hcorn.at[2]), (se, hcorn.at[3]),
        (pup_up, hpv.at[0]), (pup_down, hpv.at[1]), (pup_west, hph.at[0]), (pup_east, hph.at[1]),
    ]
    loads = [
        pltpu.make_async_copy(src, dst, band_sem.at[n]) for n, (src, dst) in enumerate(loads)
    ]
    for c in loads:
        c.start()

    def zero_acc(seg):
        def zero(i, _):
            r = pl.multiple_of(i * 8, 8)
            for p in range(2):
                for t in range(edge // LANES):
                    acc[seg, p, t, pl.ds(r, 8), :] = jnp.zeros((8, LANES), F32)
            return 0

        lax.fori_loop(0, edge // 8, zero, 0)
        for p in range(2):
            pgrad[p, :, pl.ds(pl.multiple_of(seg * pw, LANES), pw)] = jnp.zeros((pw, pw), F32)

    def own_terms(seg):
        wl = jnp.where(seg == 0, w_left, 1.0)
        wr = jnp.where(seg == cols_dev - 1, w_right, 1.0)
        il = jnp.where(seg == 0, 0.0, 1.0)
        ir = jnp.where(seg == cols_dev - 1, 0.0, 1.0)
        lo_nb = jnp.maximum(2 * seg - 1, 0)
        hi_nb = jnp.minimum(2 * seg + 2, 2 * cols_dev - 1)
        cbase = pl.multiple_of(seg * edge, LANES)

        def side(i, _):
            r = pl.multiple_of(i * SUB, SUB)
            vert = 1.0 + jnp.where(r < band, w_top, 0.0) + jnp.where(r >= edge - band, w_bot, 0.0)
            for p in range(2):
                mine = sides[2 * seg, p, pl.ds(r, SUB), :].astype(F32)
                other = sides[lo_nb, p, pl.ds(r, SUB), :].astype(F32)
                acc[seg, p, 0, pl.ds(r, SUB), :] += MU_WEIGHT * (wl * vert * mine - il * other)
                mine = sides[2 * seg + 1, p, pl.ds(r, SUB), :].astype(F32)
                other = sides[hi_nb, p, pl.ds(r, SUB), :].astype(F32)
                acc[seg, p, last, pl.ds(r, SUB), :] += MU_WEIGHT * (
                    wr * vert * mine - ir * other
                )
            return 0

        lax.fori_loop(0, edge // SUB, side, 0)

        def flat(i, _):
            r = pl.multiple_of(i * SUB, SUB)
            for p in range(2):
                for j, w in ((0, w_top), (1, w_bot)):
                    mine = rows_buf[j, p, pl.ds(r, SUB), pl.ds(cbase, edge)].astype(F32)
                    rs = pl.ds(pl.multiple_of(r + j * (edge - band), SUB), SUB)
                    for t in range(edge // LANES):
                        acc[seg, p, t, rs, :] += (MU_WEIGHT * w) * mine[
                            :, t * LANES : (t + 1) * LANES
                        ]
            return 0

        lax.fori_loop(0, band // SUB, flat, 0)
        pc = pl.multiple_of(seg * pw, LANES)
        pl_c = pl.multiple_of(jnp.maximum(seg - 1, 0) * pw, LANES)
        pr_c = pl.multiple_of(jnp.minimum(seg + 1, cols_dev - 1) * pw, LANES)
        near = w_top + w_bot + wl + wr

        def pups(i, _):
            r = pl.multiple_of(i * SUB, SUB)
            for p in range(2):
                mine = pup[p, pl.ds(r, SUB), pl.ds(pc, pw)].astype(F32)
                lef = pup[p, pl.ds(r, SUB), pl.ds(pl_c, pw)].astype(F32)
                rig = pup[p, pl.ds(r, SUB), pl.ds(pr_c, pw)].astype(F32)
                pgrad[p, pl.ds(r, SUB), pl.ds(pc, pw)] += LAM_WEIGHT * (
                    near * mine - il * lef - ir * rig
                )
            return 0

        lax.fori_loop(0, pw // SUB, pups, 0)

    def halo_terms(seg):
        def rows_part(j, edge_row):
            def step(i, _):
                r = pl.multiple_of(i * SUB, SUB)
                rs = pl.ds(pl.multiple_of(r + edge_row, SUB), SUB)
                for p in range(2):
                    cb = pl.multiple_of(seg * edge, LANES)
                    wide = hrows[j, p, pl.ds(r, SUB), pl.ds(cb, edge)].astype(F32)
                    for t in range(last + 1):
                        acc[seg, p, t, rs, :] -= MU_WEIGHT * wide[:, t * LANES : (t + 1) * LANES]
                return 0

            lax.fori_loop(0, band // SUB, step, 0)

            def corner(t, fetch):
                for p in range(2):
                    for r in range(0, band, SUB):
                        rs = slice(edge_row + r, edge_row + r + SUB)
                        acc[seg, p, t, rs, :] -= MU_WEIGHT * fetch(p, slice(r, r + SUB)).astype(F32)

            @pl.when(seg > 0)
            def _():
                c0 = pl.multiple_of(seg * edge - LANES, LANES)
                corner(0, lambda p, r: hrows[j, p, r, pl.ds(c0, LANES)])

            @pl.when(seg < cols_dev - 1)
            def _():
                c0 = pl.multiple_of((seg + 1) * edge, LANES)
                corner(last, lambda p, r: hrows[j, p, r, pl.ds(c0, LANES)])

            @pl.when((seg == 0) & (w_left > 0.0))
            def _():
                corner(0, lambda p, r: hcorn[2 * j, p, r, :])

            @pl.when((seg == cols_dev - 1) & (w_right > 0.0))
            def _():
                corner(last, lambda p, r: hcorn[2 * j + 1, p, r, :])

            pc = pl.multiple_of(seg * pw, LANES)
            for p in range(2):
                for r in range(0, pw, CH):
                    rows = slice(r, r + CH)
                    pgrad[p, rows, pl.ds(pc, pw)] -= LAM_WEIGHT * hpv[
                        j, p, rows, pl.ds(pc, pw)
                    ].astype(F32)

        def cols_part(j, t):
            def step(i, _):
                rs = pl.ds(pl.multiple_of(i * CH, CH), CH)
                for p in range(2):
                    acc[seg, p, t, rs, :] -= MU_WEIGHT * hsides[j, p, rs, :].astype(F32)
                return 0

            lax.fori_loop(0, edge // CH, step, 0)
            pc = pl.multiple_of(seg * pw, LANES)
            for p in range(2):
                for r in range(0, pw, CH):
                    rows = slice(r, r + CH)
                    pgrad[p, rows, pl.ds(pc, pw)] -= LAM_WEIGHT * hph[j, p, rows, :].astype(F32)

        @pl.when(w_top > 0.0)
        def _():
            rows_part(0, 0)

        @pl.when(w_bot > 0.0)
        def _():
            rows_part(1, edge - band)

        @pl.when((seg == 0) & (w_left > 0.0))
        def _():
            cols_part(0, 0)

        @pl.when((seg == cols_dev - 1) & (w_right > 0.0))
        def _():
            cols_part(1, last)

    def slot_step(seg, slot):
        a, b, _, b_al = window_of(start_ref, seg, slot, edge, win_r, win_c)
        b_off = b - b_al
        tile0 = b_al // LANES
        pc = pl.multiple_of(seg * pw, LANES)
        n = seg * MAXL + slot
        for r in range(0, pw, CH):
            rows = slice(r, r + CH)
            bre, bim = backs[n, 0, rows, :], backs[n, 1, rows, :]
            pre = pup[0, rows, pl.ds(pc, pw)].astype(F32)
            pim = pup[1, rows, pl.ds(pc, pw)].astype(F32)
            cre, cim = crops[n, 0, rows, :].astype(F32), crops[n, 1, rows, :].astype(F32)
            pgrad[0, rows, pl.ds(pc, pw)] += cre * bre + cim * bim
            pgrad[1, rows, pl.ds(pc, pw)] += cre * bim - cim * bre
            blank = jnp.zeros((CH, win_c - pw), F32)
            for p, val in ((0, pre * bre + pim * bim), (1, pre * bim - pim * bre)):
                wide = pltpu.roll(jnp.concatenate([val, blank], axis=1), b_off, axis=1)
                for t in range(win_t):
                    acc[seg, p, tile0 + t, pl.ds(a + r, CH), :] += wide[
                        :, t * LANES : (t + 1) * LANES
                    ]

    def put_out(seg):
        cb = pl.multiple_of(seg * edge, LANES)
        return pltpu.make_async_copy(
            stage.at[seg], out.at[:, :, pl.ds(cb, edge)], out_sem.at[seg]
        )

    def segment(seg, _):
        zero_acc(seg)

        @pl.when(seg == 0)
        def _():
            for c in loads:
                c.wait()

        own_terms(seg)
        halo_terms(seg)

        def one(slot, _):
            slot_step(seg, slot)
            return 0

        lax.fori_loop(0, count_ref[seg], one, 0)

        def conv(i, _):
            rs = pl.ds(pl.multiple_of(i * SUB, SUB), SUB)
            for p in range(2):
                for t in range(edge // LANES):
                    stage[seg, p, rs, t * LANES : (t + 1) * LANES] = acc[
                        seg, p, t, rs, :
                    ].astype(BF16)
            return 0

        lax.fori_loop(0, edge // SUB, conv, 0)
        put_out(seg).start()
        return 0

    lax.fori_loop(0, cols_dev, segment, 0)
    for s in range(cols_dev):
        put_out(s).wait()


def local(spectrum, pupils, amplitudes, crop_starts, led_counts):
    cols_dev = amplitudes.shape[1]
    total = cols_dev * MAXL
    pw = pupils.shape[1]
    edge = spectrum.shape[1]
    width = spectrum.shape[2]
    pwide = pupils.shape[2]
    band = 2 * H
    iy, ix = lax.axis_index("sy"), lax.axis_index("sx")
    flags = jnp.stack(
        [iy > 0, iy < lax.axis_size("sy") - 1, ix > 0, ix < lax.axis_size("sx") - 1]
    ).astype(F32)
    table = jnp.asarray(half_tables(pw))
    smem = pl.BlockSpec(memory_space=pltpu.SMEM)
    vmem = pl.BlockSpec(memory_space=pltpu.VMEM)
    hbm = pl.BlockSpec(memory_space=pltpu.HBM)
    win_r, win_c = pw + SUB, pw + LANES
    starts = crop_starts.reshape(-1)
    counts = led_counts.reshape(-1)
    sds = jax.ShapeDtypeStruct
    crops = pl.pallas_call(
        crop_kernel,
        out_shape=sds((total, 2, pw, pw), BF16),
        in_specs=[smem, smem, hbm],
        out_specs=vmem,
        scratch_shapes=[
            pltpu.VMEM((2, 2, win_r, win_c), BF16),
            pltpu.VMEM((2, win_c // LANES, win_r, LANES), F32),
            pltpu.SemaphoreType.DMA((2,)),
        ],
        compiler_params=pltpu.CompilerParams(vmem_limit_bytes=16 * 2**20),
        name="crops",
    )(starts, counts, spectrum)
    rows_s, cols_s = sds((2, band, width), BF16), sds((2, edge, band), BF16)
    pv_s, ph_s, corner_s = sds(pupils.shape, BF16), sds((2, pw, pw), BF16), sds((2, band, band), BF16)
    halos = (rows_s, rows_s, cols_s, cols_s, pv_s, pv_s, ph_s, ph_s) + (corner_s,) * 4
    backs, *around = pl.pallas_call(
        wave_kernel,
        out_shape=(sds((total, 2, pw, pw), F32),) + halos,
        in_specs=[hbm, hbm, hbm, vmem, vmem, vmem],
        out_specs=(vmem,) + (hbm,) * len(halos),
        scratch_shapes=[
            pltpu.VMEM((2, pw // LANES, pw, LANES), F32),
            pltpu.VMEM((4, 2, pw, pw), BF16),
            pltpu.VMEM((4, pw, pw), F32),
            pltpu.VMEM((pw, pw), F32),
            pltpu.SemaphoreType.DMA((pw // LANES, 2)),
            pltpu.SemaphoreType.DMA((len(halos),)),
            pltpu.SemaphoreType.DMA((len(halos),)),
        ],
        compiler_params=pltpu.CompilerParams(
            vmem_limit_bytes=24 * 2**20, collective_id=0, has_side_effects=True
        ),
        name="waves",
    )(spectrum, pupils, amplitudes[0], crops, pupils, table)
    return pl.pallas_call(
        finish_kernel,
        out_shape=(sds(spectrum.shape, BF16), sds(pupils.shape, F32)),
        in_specs=[smem, smem, smem, hbm, vmem, vmem, vmem] + [hbm] * len(halos),
        out_specs=(hbm, vmem),
        scratch_shapes=[
            pltpu.VMEM((cols_dev, 2, edge // LANES, edge, LANES), F32),
            pltpu.VMEM((cols_dev, 2, edge, edge), BF16),
            pltpu.VMEM((2, 2, band, width), BF16),
            pltpu.VMEM((2 * cols_dev, 2, edge, band), BF16),
            pltpu.VMEM((2,) + rows_s.shape, BF16),
            pltpu.VMEM((2,) + cols_s.shape, BF16),
            pltpu.VMEM((4,) + corner_s.shape, BF16),
            pltpu.VMEM((2,) + pv_s.shape, BF16),
            pltpu.VMEM((2,) + ph_s.shape, BF16),
            pltpu.SemaphoreType.DMA((2 + 2 * cols_dev + len(halos),)),
            pltpu.SemaphoreType.DMA((cols_dev,)),
        ],
        compiler_params=pltpu.CompilerParams(vmem_limit_bytes=52 * 2**20),
        name="finish",
    )(starts, counts, flags, spectrum, pupils, crops, backs, *around)


def solution(mesh):
    placed = (
        P(None, "sy", "sx"),
        P(None, "sy", "sx"),
        P("sy", "sx", None, None, None),
        P("sy", "sx", None, None),
        P("sy", "sx"),
    )
    return jax.shard_map(
        local,
        mesh=mesh,
        in_specs=placed,
        out_specs=(P(None, "sy", "sx"), P(None, "sy", "sx")),
        check_vma=False,
    )
```

```python
import functools
import math

import jax
import jax.numpy as jnp
import numpy as np
from jax import lax
from jax.experimental import pallas as pl
from jax.experimental.pallas import tpu as pltpu
from jax.sharding import PartitionSpec as P

H = 64
MAXL = 4
LANES = 128
CH = 32
GRANT = 62 * 2**20
SUB = 16
FLOOR_SQUARE = 0.0625
MU_WEIGHT = 0.5
LAM_WEIGHT = 0.5
F32 = jnp.float32
BF16 = jnp.bfloat16

def half_tables(side):
    half = side // 2
    n = np.arange(half)[:, None]
    k = np.arange(half)[None, :]
    mats = []
    for odd in (0, 1):
        ang = 2.0 * math.pi * ((n * (2 * k + odd)) % side) / side
        re, im = np.cos(ang) / math.sqrt(side), np.sin(ang) / math.sqrt(side)
        right = np.block([[re, im], [-im, re]])
        mats += [right, right.T]
    mats = np.stack(mats).astype(np.float32)
    hi = mats.astype(jnp.bfloat16)
    lo = (mats - hi.astype(np.float32)).astype(jnp.bfloat16)
    perm = np.zeros((side, side), np.float32)
    perm[2 * np.arange(half), np.arange(half)] = 1.0
    perm[2 * np.arange(half) + 1, half + np.arange(half)] = 1.0
    return np.concatenate([hi, lo, perm.astype(jnp.bfloat16)[None]])


def split(value):
    hi = value.astype(BF16)
    return hi, (value - hi.astype(F32)).astype(BF16)


def dot(a, b):
    return jnp.dot(a, b, preferred_element_type=F32)


def window_of(start_ref, seg, slot, edge, win_r, win_c):
    base = (seg * MAXL + slot) * 2
    a = start_ref[base]
    b = start_ref[base + 1]
    a_al = jnp.minimum(a // SUB * SUB, edge - win_r)
    b_al = jnp.minimum(b // LANES * LANES, edge - win_c)
    return a, b, a_al, b_al


def crop_kernel(start_ref, count_ref, spec, crops, win, wf, in_sem):
    pw = crops.shape[2]
    edge = spec.shape[1]
    cols_dev = spec.shape[2] // edge
    win_r, win_c = win.shape[2], win.shape[3]
    win_t = win_c // LANES

    def fetch(seg, slot, buf):
        _, _, a_al, b_al = window_of(start_ref, seg, slot, edge, win_r, win_c)
        rs = pl.multiple_of(a_al, SUB)
        cs = pl.multiple_of(seg * edge + b_al, LANES)
        return pltpu.make_async_copy(
            spec.at[:, pl.ds(rs, win_r), pl.ds(cs, win_c)], win.at[buf], in_sem.at[buf]
        )

    fetch(0, 0, 0).start()

    def slot_step(seg, slot, count):
        buf = lax.rem(count, 2)
        more = slot + 1 < count_ref[seg]
        nseg = jnp.where(more, seg, seg + 1)
        nslot = jnp.where(more, slot + 1, 0)

        @pl.when(nseg < cols_dev)
        def _():
            fetch(nseg, nslot, 1 - buf).start()

        fetch(seg, slot, buf).wait()
        a, b, a_al, b_al = window_of(start_ref, seg, slot, edge, win_r, win_c)
        a_off = a - a_al
        for p in range(2):
            for r in range(0, win_r, SUB):
                wide = win[buf, p, r : r + SUB, :].astype(F32)
                for t in range(win_t):
                    wf[p, t, r : r + SUB, :] = wide[:, t * LANES : (t + 1) * LANES]
        back_roll = lax.rem(win_c - (b - b_al), win_c)
        for r in range(0, pw, CH):
            for p in range(2):
                wide = jnp.concatenate(
                    [wf[p, t, pl.ds(a_off + r, CH), :] for t in range(win_t)], axis=1
                )
                crops[seg * MAXL + slot, p, r : r + CH, :] = pltpu.roll(
                    wide, back_roll, axis=1
                )[:, :pw].astype(BF16)
        return count + 1

    def segment(seg, count):
        return lax.fori_loop(
            0, count_ref[seg], lambda slot, c: slot_step(seg, slot, c), count
        )

    lax.fori_loop(0, cols_dev, segment, jnp.int32(0))


def wave_kernel(
    count_ref, flag_ref, spec, pup_hbm, amps, crops, pup, tab,
    pgrad, backs, up, down, west, east, pup_up, pup_down, pup_west, pup_east, nw, ne, sw, se,
    ampbuf, cbuf, obuf, xs, ys, ampp, in_sem, back_sem, send_sem, recv_sem,
):
    pw = pup.shape[1]
    half = pw // 2
    edge = spec.shape[1]
    width = spec.shape[2]
    pwide = pup.shape[2]
    band = 2 * H
    total = crops.shape[0]
    iy, ix = lax.axis_index("sy"), lax.axis_index("sx")
    ny, nx = lax.axis_size("sy"), lax.axis_size("sx")
    has = {}
    for dy in (-1, 0, 1):
        for dx in (-1, 0, 1):
            ok = (iy + dy >= 0) & (iy + dy < ny) & (ix + dx >= 0) & (ix + dx < nx)
            has[dy, dx] = ok

    barrier = pltpu.get_barrier_semaphore()
    near = [(dy, dx) for dy in (-1, 0, 1) for dx in (-1, 0, 1) if dy or dx]
    for dy, dx in near:
        @pl.when(has[dy, dx])
        def _(dy=dy, dx=dx):
            pl.semaphore_signal(
                barrier, inc=1, device_id=(iy + dy, ix + dx),
                device_id_type=pl.DeviceIdType.MESH,
            )
    pl.semaphore_wait(barrier, sum(has[d].astype(jnp.int32) for d in near))
    tops, bots = slice(0, band), slice(edge - band, edge)
    lefts, rights = slice(0, band), slice(width - band, width)
    moves = [
        ((1, 0), spec.at[:, bots, :], up),
        ((-1, 0), spec.at[:, tops, :], down),
        ((0, 1), spec.at[:, :, rights], west),
        ((0, -1), spec.at[:, :, lefts], east),
        ((1, 0), pup_hbm, pup_up),
        ((-1, 0), pup_hbm, pup_down),
        ((0, 1), pup_hbm.at[:, :, pwide - pw :], pup_west),
        ((0, -1), pup_hbm.at[:, :, :pw], pup_east),
        ((1, 1), spec.at[:, bots, rights], nw),
        ((1, -1), spec.at[:, bots, lefts], ne),
        ((-1, 1), spec.at[:, tops, rights], sw),
        ((-1, -1), spec.at[:, tops, lefts], se),
    ]
    copies = []
    for n, ((dy, dx), src, dst) in enumerate(moves):
        copies.append(
            pltpu.make_async_remote_copy(
                src_ref=src, dst_ref=dst, send_sem=send_sem.at[n], recv_sem=recv_sem.at[n],
                device_id=(iy + dy, ix + dx), device_id_type=pl.DeviceIdType.MESH,
            )
        )
    for c, ((dy, dx), _, _) in zip(copies, moves):
        @pl.when(has[dy, dx])
        def _(c=c):
            c.start()

    def put(which, rows, cols, value):
        hi, lo = split(value)
        xs[which, 0, rows, cols] = hi
        xs[which, 1, rows, cols] = lo

    def from_right(which, table):
        lhs = jnp.concatenate([xs[which, 0], xs[which, 1], xs[which, 0]], axis=1)
        rhs = jnp.concatenate([tab[table], tab[table], tab[4 + table]], axis=0)
        ys[which] = dot(lhs, rhs)

    def from_left(which, table):
        rhs = jnp.concatenate([xs[which, 0], xs[which, 1], xs[which, 0]], axis=0)
        lhs = jnp.concatenate([tab[table], tab[table], tab[4 + table]], axis=1)
        ys[which] = dot(lhs, rhs)

    lo_c, hi_c, all_c = slice(0, half), slice(half, pw), slice(0, pw)

    def fetch(i, buf):
        seg = lax.div(i, MAXL)
        slot = lax.rem(i, MAXL)
        return [
            pltpu.make_async_copy(
                amps.at[seg, slot, :, t * LANES : (t + 1) * LANES],
                ampbuf.at[buf, t],
                in_sem.at[t, buf],
            )
            for t in range(pw // LANES)
        ] + [pltpu.make_async_copy(crops.at[i], cbuf.at[buf], in_sem.at[pw // LANES, buf])]

    def give(i, buf):
        return pltpu.make_async_copy(obuf.at[buf], backs.at[i], back_sem.at[buf])

    for c in fetch(0, 0):
        c.start()
    cols_dev = width // edge
    w_top, w_bot, w_left, w_right = (flag_ref[k] for k in range(4))

    def own_pup(seg, _):
        wl = jnp.where(seg == 0, w_left, 1.0)
        wr = jnp.where(seg == cols_dev - 1, w_right, 1.0)
        il = jnp.where(seg == 0, 0.0, 1.0)
        ir = jnp.where(seg == cols_dev - 1, 0.0, 1.0)
        pc = pl.multiple_of(seg * pw, LANES)
        pl_c = pl.multiple_of(jnp.maximum(seg - 1, 0) * pw, LANES)
        pr_c = pl.multiple_of(jnp.minimum(seg + 1, cols_dev - 1) * pw, LANES)
        near = w_top + w_bot + wl + wr

        def pups(i, _):
            r = pl.multiple_of(i * SUB, SUB)
            for p in range(2):
                mine = pup[p, pl.ds(r, SUB), pl.ds(pc, pw)].astype(F32)
                lef = pup[p, pl.ds(r, SUB), pl.ds(pl_c, pw)].astype(F32)
                rig = pup[p, pl.ds(r, SUB), pl.ds(pr_c, pw)].astype(F32)
                pgrad[p, pl.ds(r, SUB), pl.ds(pc, pw)] = LAM_WEIGHT * (
                    near * mine - il * lef - ir * rig
                )
            return 0

        lax.fori_loop(0, pw // SUB, pups, 0)
        return 0

    lax.fori_loop(0, cols_dev, own_pup, 0)

    def slot_step(i, _):
        buf = lax.rem(i, 2)

        @pl.when(i + 1 < total)
        def _():
            for c in fetch(i + 1, 1 - buf):
                c.start()

        for c in fetch(i, buf):
            c.wait()
        pc = pl.multiple_of(lax.div(i, MAXL) * pw, LANES)
        for r in range(0, pw, CH):
            rows = slice(r, r + CH)
            cre = cbuf[buf, 0, rows, :].astype(F32)
            cim = cbuf[buf, 1, rows, :].astype(F32)
            pre = pup[0, rows, pl.ds(pc, pw)].astype(F32)
            pim = pup[1, rows, pl.ds(pc, pw)].astype(F32)
            fre = pre * cre - pim * cim
            fim = pre * cim + pim * cre
            put(0, rows, lo_c, fre[:, lo_c] + fre[:, hi_c])
            put(0, rows, hi_c, fim[:, lo_c] + fim[:, hi_c])
            put(1, rows, lo_c, fre[:, lo_c] - fre[:, hi_c])
            put(1, rows, hi_c, fim[:, lo_c] - fim[:, hi_c])
        from_right(0, 0)
        from_right(1, 2)
        for r in range(0, half, CH):
            for part, cols in ((0, lo_c), (1, hi_c)):
                rows = slice(part * half + r, part * half + r + CH)
                for which, ocols in ((0, lo_c), (1, hi_c)):
                    upper = ys[which, r : r + CH, cols]
                    lower = ys[which, half + r : half + r + CH, cols]
                    put(2, rows, ocols, upper + lower)
                    put(3, rows, ocols, upper - lower)
        ahi, alo = [], []
        for odd in range(2):
            h, l = split(
                jnp.concatenate(
                    [ampbuf[buf, t, pl.ds(odd, half, stride=2), :] for t in range(pw // LANES)],
                    axis=1,
                )
            )
            ahi.append(h)
            alo.append(l)
        lhs = jnp.concatenate(
            [jnp.concatenate(ahi, axis=0), jnp.concatenate(alo, axis=0)], axis=1
        )
        ampp[...] = dot(lhs, jnp.concatenate([tab[8], tab[8]], axis=0))
        from_left(2, 1)
        from_left(3, 3)
        for which in range(2):
            for r in range(0, half, CH):
                re = ys[2 + which, r : r + CH, :]
                im = ys[2 + which, half + r : half + r + CH, :]
                amp = ampp[which * half + r : which * half + r + CH, :]
                keep = 1.0 - amp * lax.rsqrt(jnp.maximum(re * re + im * im, FLOOR_SQUARE))
                put(which, slice(r, r + CH), all_c, re * keep)
                put(which, slice(half + r, half + r + CH), all_c, im * keep)
        from_left(0, 0)
        from_left(1, 2)
        for r in range(0, half, CH):
            for part, cols in ((0, lo_c), (1, hi_c)):
                even = ys[0, part * half + r : part * half + r + CH, :]
                odd = ys[1, part * half + r : part * half + r + CH, :]
                upper, lower = even + odd, even - odd
                for rows, val in (
                    (slice(r, r + CH), upper), (slice(half + r, half + r + CH), lower),
                ):
                    put(2, rows, cols, val[:, lo_c])
                    put(3, rows, cols, val[:, hi_c])
        from_right(2, 1)
        from_right(3, 3)
        @pl.when(i >= 2)
        def _():
            give(i - 2, buf).wait()

        live = jnp.full((CH, pw), lax.rem(i, MAXL), jnp.int32) < count_ref[lax.div(i, MAXL)]
        for r in range(0, pw, CH):
            rows = slice(r, r + CH)
            even, odd = ys[2, rows, :], ys[3, rows, :]
            plus, minus = even + odd, even - odd
            bre = jnp.concatenate([plus[:, lo_c], minus[:, lo_c]], axis=1)
            bim = jnp.concatenate([plus[:, hi_c], minus[:, hi_c]], axis=1)
            pre = pup[0, rows, pl.ds(pc, pw)].astype(F32)
            pim = pup[1, rows, pl.ds(pc, pw)].astype(F32)
            cre = cbuf[buf, 0, rows, :].astype(F32)
            cim = cbuf[buf, 1, rows, :].astype(F32)
            obuf[buf, 0, rows, :] = pre * bre + pim * bim
            obuf[buf, 1, rows, :] = pre * bim - pim * bre
            pgrad[0, rows, pl.ds(pc, pw)] += jnp.where(live, cre * bre + cim * bim, 0.0)
            pgrad[1, rows, pl.ds(pc, pw)] += jnp.where(live, cre * bim - cim * bre, 0.0)
        give(i, buf).start()
        return 0

    lax.fori_loop(0, total, slot_step, 0)
    for i in range(max(total - 2, 0), total):
        give(i, i % 2).wait()
    for c, ((dy, dx), _, _) in zip(copies, moves):
        @pl.when(has[dy, dx])
        def _(c=c):
            c.wait_send()

        @pl.when(has[-dy, -dx])
        def _(c=c):
            c.wait_recv()


def finish_kernel(
    start_ref, count_ref, flag_ref, spec, pgrad_in, backs_hbm,
    up, down, west, east, pup_up, pup_down, pup_west, pup_east, nw, ne, sw, se,
    out, pgrad,
    acc, stage, backs, rows_buf, sides, hrows, hsides, hcorn, hpv, hph, band_sem, out_sem,
):
    pw = pgrad.shape[1]
    edge = spec.shape[1]
    cols_dev = spec.shape[2] // edge
    band = 2 * H
    win_r, win_c = pw + SUB, pw + LANES
    win_t = win_c // LANES
    last = edge // LANES - 1
    w_top, w_bot, w_left, w_right = (flag_ref[i] for i in range(4))
    loads = [
        (spec.at[:, 0:band, :], rows_buf.at[0]),
        (spec.at[:, edge - band :, :], rows_buf.at[1]),
    ]
    for s in range(cols_dev):
        for j, c0 in enumerate((s * edge, (s + 1) * edge - band)):
            loads.append((spec.at[:, :, c0 : c0 + band], sides.at[2 * s + j]))
    loads += [
        (up, hrows.at[0]), (down, hrows.at[1]), (west, hsides.at[0]), (east, hsides.at[1]),
        (nw, hcorn.at[0]), (ne, hcorn.at[1]), (sw, hcorn.at[2]), (se, hcorn.at[3]),
        (pup_up, hpv.at[0]), (pup_down, hpv.at[1]), (pup_west, hph.at[0]), (pup_east, hph.at[1]),
        (backs_hbm, backs),
    ]
    loads = [
        pltpu.make_async_copy(src, dst, band_sem.at[n]) for n, (src, dst) in enumerate(loads)
    ]
    for c in loads:
        c.start()

    def zero_acc(seg):
        def zero(i, _):
            r = pl.multiple_of(i * 8, 8)
            for p in range(2):
                for t in range(edge // LANES):
                    acc[seg, p, t, pl.ds(r, 8), :] = jnp.zeros((8, LANES), F32)
            return 0

        lax.fori_loop(0, edge // 8, zero, 0)

    def own_terms(seg):
        wl = jnp.where(seg == 0, w_left, 1.0)
        wr = jnp.where(seg == cols_dev - 1, w_right, 1.0)
        il = jnp.where(seg == 0, 0.0, 1.0)
        ir = jnp.where(seg == cols_dev - 1, 0.0, 1.0)
        lo_nb = jnp.maximum(2 * seg - 1, 0)
        hi_nb = jnp.minimum(2 * seg + 2, 2 * cols_dev - 1)
        cbase = pl.multiple_of(seg * edge, LANES)

        def side(i, _):
            r = pl.multiple_of(i * SUB, SUB)
            vert = 1.0 + jnp.where(r < band, w_top, 0.0) + jnp.where(r >= edge - band, w_bot, 0.0)
            for p in range(2):
                mine = sides[2 * seg, p, pl.ds(r, SUB), :].astype(F32)
                other = sides[lo_nb, p, pl.ds(r, SUB), :].astype(F32)
                acc[seg, p, 0, pl.ds(r, SUB), :] += MU_WEIGHT * (wl * vert * mine - il * other)
                mine = sides[2 * seg + 1, p, pl.ds(r, SUB), :].astype(F32)
                other = sides[hi_nb, p, pl.ds(r, SUB), :].astype(F32)
                acc[seg, p, last, pl.ds(r, SUB), :] += MU_WEIGHT * (
                    wr * vert * mine - ir * other
                )
            return 0

        lax.fori_loop(0, edge // SUB, side, 0)

        def flat(i, _):
            r = pl.multiple_of(i * SUB, SUB)
            for p in range(2):
                for j, w in ((0, w_top), (1, w_bot)):
                    mine = rows_buf[j, p, pl.ds(r, SUB), pl.ds(cbase, edge)].astype(F32)
                    rs = pl.ds(pl.multiple_of(r + j * (edge - band), SUB), SUB)
                    for t in range(edge // LANES):
                        acc[seg, p, t, rs, :] += (MU_WEIGHT * w) * mine[
                            :, t * LANES : (t + 1) * LANES
                        ]
            return 0

        lax.fori_loop(0, band // SUB, flat, 0)

    def halo_terms(seg):
        def rows_part(j, edge_row):
            def step(i, _):
                r = pl.multiple_of(i * SUB, SUB)
                rs = pl.ds(pl.multiple_of(r + edge_row, SUB), SUB)
                for p in range(2):
                    cb = pl.multiple_of(seg * edge, LANES)
                    wide = hrows[j, p, pl.ds(r, SUB), pl.ds(cb, edge)].astype(F32)
                    for t in range(last + 1):
                        acc[seg, p, t, rs, :] -= MU_WEIGHT * wide[:, t * LANES : (t + 1) * LANES]
                return 0

            lax.fori_loop(0, band // SUB, step, 0)

            def corner(t, fetch):
                for p in range(2):
                    for r in range(0, band, SUB):
                        rs = slice(edge_row + r, edge_row + r + SUB)
                        acc[seg, p, t, rs, :] -= MU_WEIGHT * fetch(p, slice(r, r + SUB)).astype(F32)

            @pl.when(seg > 0)
            def _():
                c0 = pl.multiple_of(seg * edge - LANES, LANES)
                corner(0, lambda p, r: hrows[j, p, r, pl.ds(c0, LANES)])

            @pl.when(seg < cols_dev - 1)
            def _():
                c0 = pl.multiple_of((seg + 1) * edge, LANES)
                corner(last, lambda p, r: hrows[j, p, r, pl.ds(c0, LANES)])

            @pl.when((seg == 0) & (w_left > 0.0))
            def _():
                corner(0, lambda p, r: hcorn[2 * j, p, r, :])

            @pl.when((seg == cols_dev - 1) & (w_right > 0.0))
            def _():
                corner(last, lambda p, r: hcorn[2 * j + 1, p, r, :])

            pc = pl.multiple_of(seg * pw, LANES)
            for p in range(2):
                for r in range(0, pw, CH):
                    rows = slice(r, r + CH)
                    pgrad[p, rows, pl.ds(pc, pw)] -= LAM_WEIGHT * hpv[
                        j, p, rows, pl.ds(pc, pw)
                    ].astype(F32)

        def cols_part(j, t):
            def step(i, _):
                rs = pl.ds(pl.multiple_of(i * CH, CH), CH)
                for p in range(2):
                    acc[seg, p, t, rs, :] -= MU_WEIGHT * hsides[j, p, rs, :].astype(F32)
                return 0

            lax.fori_loop(0, edge // CH, step, 0)
            pc = pl.multiple_of(seg * pw, LANES)
            for p in range(2):
                for r in range(0, pw, CH):
                    rows = slice(r, r + CH)
                    pgrad[p, rows, pl.ds(pc, pw)] -= LAM_WEIGHT * hph[j, p, rows, :].astype(F32)

        @pl.when(w_top > 0.0)
        def _():
            rows_part(0, 0)

        @pl.when(w_bot > 0.0)
        def _():
            rows_part(1, edge - band)

        @pl.when((seg == 0) & (w_left > 0.0))
        def _():
            cols_part(0, 0)

        @pl.when((seg == cols_dev - 1) & (w_right > 0.0))
        def _():
            cols_part(1, last)

    def slot_step(seg, slot):
        a, b, _, b_al = window_of(start_ref, seg, slot, edge, win_r, win_c)
        b_off = b - b_al
        tile0 = b_al // LANES
        n = seg * MAXL + slot
        for r in range(0, pw, CH):
            rows = slice(r, r + CH)
            blank = jnp.zeros((CH, win_c - pw), F32)
            for p in range(2):
                val = backs[n, p, rows, :]
                wide = pltpu.roll(jnp.concatenate([val, blank], axis=1), b_off, axis=1)
                for t in range(win_t):
                    acc[seg, p, tile0 + t, pl.ds(a + r, CH), :] += wide[
                        :, t * LANES : (t + 1) * LANES
                    ]

    def put_out(seg):
        cb = pl.multiple_of(seg * edge, LANES)
        return pltpu.make_async_copy(
            stage.at[seg], out.at[:, :, pl.ds(cb, edge)], out_sem.at[seg]
        )

    for s in range(cols_dev):
        zero_acc(s)
    pgrad[...] = pgrad_in[...]
    for c in loads:
        c.wait()

    def segment(seg, _):
        own_terms(seg)
        halo_terms(seg)

        def one(slot, _):
            slot_step(seg, slot)
            return 0

        lax.fori_loop(0, count_ref[seg], one, 0)

        def conv(i, _):
            rs = pl.ds(pl.multiple_of(i * SUB, SUB), SUB)
            for p in range(2):
                for t in range(edge // LANES):
                    stage[seg, p, rs, t * LANES : (t + 1) * LANES] = acc[
                        seg, p, t, rs, :
                    ].astype(BF16)
            return 0

        lax.fori_loop(0, edge // SUB, conv, 0)
        put_out(seg).start()
        return 0

    lax.fori_loop(0, cols_dev, segment, 0)
    for s in range(cols_dev):
        put_out(s).wait()


def local(spectrum, pupils, amplitudes, crop_starts, led_counts):
    cols_dev = amplitudes.shape[1]
    total = cols_dev * MAXL
    pw = pupils.shape[1]
    edge = spectrum.shape[1]
    width = spectrum.shape[2]
    pwide = pupils.shape[2]
    band = 2 * H
    iy, ix = lax.axis_index("sy"), lax.axis_index("sx")
    flags = jnp.stack(
        [iy > 0, iy < lax.axis_size("sy") - 1, ix > 0, ix < lax.axis_size("sx") - 1]
    ).astype(F32)
    table = jnp.asarray(half_tables(pw))
    smem = pl.BlockSpec(memory_space=pltpu.SMEM)
    vmem = pl.BlockSpec(memory_space=pltpu.VMEM)
    hbm = pl.BlockSpec(memory_space=pltpu.HBM)
    win_r, win_c = pw + SUB, pw + LANES
    starts = crop_starts.reshape(-1)
    counts = led_counts.reshape(-1)
    sds = jax.ShapeDtypeStruct
    crops = pl.pallas_call(
        crop_kernel,
        out_shape=sds((total, 2, pw, pw), BF16),
        in_specs=[smem, smem, hbm],
        out_specs=vmem,
        scratch_shapes=[
            pltpu.VMEM((2, 2, win_r, win_c), BF16),
            pltpu.VMEM((2, win_c // LANES, win_r, LANES), F32),
            pltpu.SemaphoreType.DMA((2,)),
        ],
        compiler_params=pltpu.CompilerParams(vmem_limit_bytes=GRANT),
        name="crops",
    )(starts, counts, spectrum)
    rows_s, cols_s = sds((2, band, width), BF16), sds((2, edge, band), BF16)
    pv_s, ph_s, corner_s = sds(pupils.shape, BF16), sds((2, pw, pw), BF16), sds((2, band, band), BF16)
    halos = (rows_s, rows_s, cols_s, cols_s, pv_s, pv_s, ph_s, ph_s) + (corner_s,) * 4
    pgrad, backs, *around = pl.pallas_call(
        wave_kernel,
        out_shape=(sds(pupils.shape, F32), sds((total, 2, pw, pw), F32)) + halos,
        in_specs=[smem, smem, hbm, hbm, hbm, hbm, vmem, vmem],
        out_specs=(vmem, hbm) + (hbm,) * len(halos),
        scratch_shapes=[
            pltpu.VMEM((2, pw // LANES, pw, LANES), F32),
            pltpu.VMEM((2, 2, pw, pw), BF16),
            pltpu.VMEM((2, 2, pw, pw), F32),
            pltpu.VMEM((4, 2, pw, pw), BF16),
            pltpu.VMEM((4, pw, pw), F32),
            pltpu.VMEM((pw, pw), F32),
            pltpu.SemaphoreType.DMA((1 + pw // LANES, 2)),
            pltpu.SemaphoreType.DMA((2,)),
            pltpu.SemaphoreType.DMA((len(halos),)),
            pltpu.SemaphoreType.DMA((len(halos),)),
        ],
        compiler_params=pltpu.CompilerParams(
            vmem_limit_bytes=GRANT, collective_id=0, has_side_effects=True
        ),
        name="waves",
    )(counts, flags, spectrum, pupils, amplitudes[0], crops, pupils, table)
    return pl.pallas_call(
        finish_kernel,
        out_shape=(sds(spectrum.shape, BF16), sds(pupils.shape, F32)),
        in_specs=[smem, smem, smem, hbm, vmem, hbm] + [hbm] * len(halos),
        out_specs=(hbm, vmem),
        scratch_shapes=[
            pltpu.VMEM((cols_dev, 2, edge // LANES, edge, LANES), F32),
            pltpu.VMEM((cols_dev, 2, edge, edge), BF16),
            pltpu.VMEM((total, 2, pw, pw), F32),
            pltpu.VMEM((2, 2, band, width), BF16),
            pltpu.VMEM((2 * cols_dev, 2, edge, band), BF16),
            pltpu.VMEM((2,) + rows_s.shape, BF16),
            pltpu.VMEM((2,) + cols_s.shape, BF16),
            pltpu.VMEM((4,) + corner_s.shape, BF16),
            pltpu.VMEM((2,) + pv_s.shape, BF16),
            pltpu.VMEM((2,) + ph_s.shape, BF16),
            pltpu.SemaphoreType.DMA((3 + 2 * cols_dev + len(halos),)),
            pltpu.SemaphoreType.DMA((cols_dev,)),
        ],
        compiler_params=pltpu.CompilerParams(vmem_limit_bytes=GRANT),
        name="finish",
    )(starts, counts, flags, spectrum, pgrad, backs, *around)


def solution(mesh):
    placed = (
        P(None, "sy", "sx"),
        P(None, "sy", "sx"),
        P("sy", "sx", None, None, None),
        P("sy", "sx", None, None),
        P("sy", "sx"),
    )
    return jax.shard_map(
        local,
        mesh=mesh,
        in_specs=placed,
        out_specs=(P(None, "sy", "sx"), P(None, "sy", "sx")),
        check_vma=False,
    )
```

```python
import functools
import math

import jax
import jax.numpy as jnp
import numpy as np
from jax import lax
from jax.experimental import pallas as pl
from jax.experimental.pallas import tpu as pltpu
from jax.sharding import PartitionSpec as P

H = 64
MAXL = 4
LANES = 128
CH = 32
PIECES = 4
GRANT = 62 * 2**20
SUB = 16
FLOOR_SQUARE = 0.0625
MU_WEIGHT = 0.5
LAM_WEIGHT = 0.5
F32 = jnp.float32
BF16 = jnp.bfloat16

def half_tables(side):
    half = side // 2
    n = np.arange(half)[:, None]
    k = np.arange(half)[None, :]
    mats = []
    for odd in (0, 1):
        ang = 2.0 * math.pi * ((n * (2 * k + odd)) % side) / side
        re, im = np.cos(ang) / math.sqrt(side), np.sin(ang) / math.sqrt(side)
        right = np.block([[re, im], [-im, re]])
        mats += [right, right.T]
    mats = np.stack(mats).astype(np.float32)
    hi = mats.astype(jnp.bfloat16)
    lo = (mats - hi.astype(np.float32)).astype(jnp.bfloat16)
    perm = np.zeros((side, side), np.float32)
    perm[2 * np.arange(half), np.arange(half)] = 1.0
    perm[2 * np.arange(half) + 1, half + np.arange(half)] = 1.0
    return np.concatenate([hi, lo, perm.astype(jnp.bfloat16)[None]])


def split(value):
    hi = value.astype(BF16)
    return hi, (value - hi.astype(F32)).astype(BF16)


def dot(a, b):
    return jnp.dot(a, b, preferred_element_type=F32)


def window_of(start_ref, seg, slot, edge, win_r, win_c):
    base = (seg * MAXL + slot) * 2
    a = start_ref[base]
    b = start_ref[base + 1]
    a_al = jnp.minimum(a // SUB * SUB, edge - win_r)
    b_al = jnp.minimum(b // LANES * LANES, edge - win_c)
    return a, b, a_al, b_al


def crop_kernel(start_ref, count_ref, spec, crops, win, wf, in_sem):
    pw = crops.shape[2]
    edge = spec.shape[1]
    cols_dev = spec.shape[2] // edge
    win_r, win_c = win.shape[2], win.shape[3]
    win_t = win_c // LANES

    def fetch(seg, slot, buf):
        _, _, a_al, b_al = window_of(start_ref, seg, slot, edge, win_r, win_c)
        rs = pl.multiple_of(a_al, SUB)
        cs = pl.multiple_of(seg * edge + b_al, LANES)
        return pltpu.make_async_copy(
            spec.at[:, pl.ds(rs, win_r), pl.ds(cs, win_c)], win.at[buf], in_sem.at[buf]
        )

    fetch(0, 0, 0).start()

    def slot_step(seg, slot, count):
        buf = lax.rem(count, 2)
        more = slot + 1 < count_ref[seg]
        nseg = jnp.where(more, seg, seg + 1)
        nslot = jnp.where(more, slot + 1, 0)

        @pl.when(nseg < cols_dev)
        def _():
            fetch(nseg, nslot, 1 - buf).start()

        fetch(seg, slot, buf).wait()
        a, b, a_al, b_al = window_of(start_ref, seg, slot, edge, win_r, win_c)
        a_off = a - a_al
        for p in range(2):
            for r in range(0, win_r, SUB):
                wide = win[buf, p, r : r + SUB, :].astype(F32)
                for t in range(win_t):
                    wf[p, t, r : r + SUB, :] = wide[:, t * LANES : (t + 1) * LANES]
        back_roll = lax.rem(win_c - (b - b_al), win_c)
        for r in range(0, pw, CH):
            for p in range(2):
                wide = jnp.concatenate(
                    [wf[p, t, pl.ds(a_off + r, CH), :] for t in range(win_t)], axis=1
                )
                crops[seg * MAXL + slot, p, r : r + CH, :] = pltpu.roll(
                    wide, back_roll, axis=1
                )[:, :pw].astype(BF16)
        return count + 1

    def segment(seg, count):
        return lax.fori_loop(
            0, count_ref[seg], lambda slot, c: slot_step(seg, slot, c), count
        )

    lax.fori_loop(0, cols_dev, segment, jnp.int32(0))


def wave_kernel(
    count_ref, flag_ref, spec, pup_hbm, amps, crops, pup, tab,
    pgrad, backs, up, down, west, east, pup_up, pup_down, pup_west, pup_east, nw, ne, sw, se,
    ampbuf, cbuf, obuf, xs, ys, ampp, in_sem, back_sem, send_sem, recv_sem,
):
    pw = pup.shape[1]
    half = pw // 2
    edge = spec.shape[1]
    width = spec.shape[2]
    pwide = pup.shape[2]
    band = 2 * H
    total = crops.shape[0]
    iy, ix = lax.axis_index("sy"), lax.axis_index("sx")
    ny, nx = lax.axis_size("sy"), lax.axis_size("sx")
    has = {}
    for dy in (-1, 0, 1):
        for dx in (-1, 0, 1):
            ok = (iy + dy >= 0) & (iy + dy < ny) & (ix + dx >= 0) & (ix + dx < nx)
            has[dy, dx] = ok

    barrier = pltpu.get_barrier_semaphore()
    near = [(dy, dx) for dy in (-1, 0, 1) for dx in (-1, 0, 1) if dy or dx]
    for dy, dx in near:
        @pl.when(has[dy, dx])
        def _(dy=dy, dx=dx):
            pl.semaphore_signal(
                barrier, inc=1, device_id=(iy + dy, ix + dx),
                device_id_type=pl.DeviceIdType.MESH,
            )
    pl.semaphore_wait(barrier, sum(has[d].astype(jnp.int32) for d in near))
    tops, bots = slice(0, band), slice(edge - band, edge)
    lefts, rights = slice(0, band), slice(width - band, width)
    moves = [
        ((1, 0), spec.at[:, bots, :], up),
        ((-1, 0), spec.at[:, tops, :], down),
        ((0, 1), spec.at[:, :, rights], west),
        ((0, -1), spec.at[:, :, lefts], east),
        ((1, 0), pup_hbm, pup_up),
        ((-1, 0), pup_hbm, pup_down),
        ((0, 1), pup_hbm.at[:, :, pwide - pw :], pup_west),
        ((0, -1), pup_hbm.at[:, :, :pw], pup_east),
        ((1, 1), spec.at[:, bots, rights], nw),
        ((1, -1), spec.at[:, bots, lefts], ne),
        ((-1, 1), spec.at[:, tops, rights], sw),
        ((-1, -1), spec.at[:, tops, lefts], se),
    ]
    copies = []
    for n, ((dy, dx), src, dst) in enumerate(moves):
        copies.append(
            pltpu.make_async_remote_copy(
                src_ref=src, dst_ref=dst, send_sem=send_sem.at[n], recv_sem=recv_sem.at[n],
                device_id=(iy + dy, ix + dx), device_id_type=pl.DeviceIdType.MESH,
            )
        )
    for c, ((dy, dx), _, _) in zip(copies, moves):
        @pl.when(has[dy, dx])
        def _(c=c):
            c.start()

    def put(which, rows, cols, value):
        hi, lo = split(value)
        xs[which, 0, rows, cols] = hi
        xs[which, 1, rows, cols] = lo

    def from_right(which, table):
        lhs = jnp.concatenate([xs[which, 0], xs[which, 1], xs[which, 0]], axis=1)
        rhs = jnp.concatenate([tab[table], tab[table], tab[4 + table]], axis=0)
        ys[which] = dot(lhs, rhs)

    def from_left(which, table):
        rhs = jnp.concatenate([xs[which, 0], xs[which, 1], xs[which, 0]], axis=0)
        lhs = jnp.concatenate([tab[table], tab[table], tab[4 + table]], axis=1)
        ys[which] = dot(lhs, rhs)

    lo_c, hi_c, all_c = slice(0, half), slice(half, pw), slice(0, pw)

    def fetch(i, buf):
        seg = lax.div(i, MAXL)
        slot = lax.rem(i, MAXL)
        return [
            pltpu.make_async_copy(
                amps.at[seg, slot, :, t * LANES : (t + 1) * LANES],
                ampbuf.at[buf, t],
                in_sem.at[t, buf],
            )
            for t in range(pw // LANES)
        ] + [pltpu.make_async_copy(crops.at[i], cbuf.at[buf], in_sem.at[pw // LANES, buf])]

    def give(i, buf):
        return pltpu.make_async_copy(obuf.at[buf], backs.at[i], back_sem.at[buf])

    for c in fetch(0, 0):
        c.start()
    cols_dev = width // edge
    w_top, w_bot, w_left, w_right = (flag_ref[k] for k in range(4))

    def own_pup(seg, _):
        wl = jnp.where(seg == 0, w_left, 1.0)
        wr = jnp.where(seg == cols_dev - 1, w_right, 1.0)
        il = jnp.where(seg == 0, 0.0, 1.0)
        ir = jnp.where(seg == cols_dev - 1, 0.0, 1.0)
        pc = pl.multiple_of(seg * pw, LANES)
        pl_c = pl.multiple_of(jnp.maximum(seg - 1, 0) * pw, LANES)
        pr_c = pl.multiple_of(jnp.minimum(seg + 1, cols_dev - 1) * pw, LANES)
        near = w_top + w_bot + wl + wr

        def pups(i, _):
            r = pl.multiple_of(i * SUB, SUB)
            for p in range(2):
                mine = pup[p, pl.ds(r, SUB), pl.ds(pc, pw)].astype(F32)
                lef = pup[p, pl.ds(r, SUB), pl.ds(pl_c, pw)].astype(F32)
                rig = pup[p, pl.ds(r, SUB), pl.ds(pr_c, pw)].astype(F32)
                pgrad[p, pl.ds(r, SUB), pl.ds(pc, pw)] = LAM_WEIGHT * (
                    near * mine - il * lef - ir * rig
                )
            return 0

        lax.fori_loop(0, pw // SUB, pups, 0)
        return 0

    lax.fori_loop(0, cols_dev, own_pup, 0)

    def slot_step(i, _):
        buf = lax.rem(i, 2)

        @pl.when(i + 1 < total)
        def _():
            for c in fetch(i + 1, 1 - buf):
                c.start()

        for c in fetch(i, buf):
            c.wait()
        pc = pl.multiple_of(lax.div(i, MAXL) * pw, LANES)
        for r in range(0, pw, CH):
            rows = slice(r, r + CH)
            cre = cbuf[buf, 0, rows, :].astype(F32)
            cim = cbuf[buf, 1, rows, :].astype(F32)
            pre = pup[0, rows, pl.ds(pc, pw)].astype(F32)
            pim = pup[1, rows, pl.ds(pc, pw)].astype(F32)
            fre = pre * cre - pim * cim
            fim = pre * cim + pim * cre
            put(0, rows, lo_c, fre[:, lo_c] + fre[:, hi_c])
            put(0, rows, hi_c, fim[:, lo_c] + fim[:, hi_c])
            put(1, rows, lo_c, fre[:, lo_c] - fre[:, hi_c])
            put(1, rows, hi_c, fim[:, lo_c] - fim[:, hi_c])
        from_right(0, 0)
        from_right(1, 2)
        for r in range(0, half, CH):
            for part, cols in ((0, lo_c), (1, hi_c)):
                rows = slice(part * half + r, part * half + r + CH)
                for which, ocols in ((0, lo_c), (1, hi_c)):
                    upper = ys[which, r : r + CH, cols]
                    lower = ys[which, half + r : half + r + CH, cols]
                    put(2, rows, ocols, upper + lower)
                    put(3, rows, ocols, upper - lower)
        ahi, alo = [], []
        for odd in range(2):
            h, l = split(
                jnp.concatenate(
                    [ampbuf[buf, t, pl.ds(odd, half, stride=2), :] for t in range(pw // LANES)],
                    axis=1,
                )
            )
            ahi.append(h)
            alo.append(l)
        lhs = jnp.concatenate(
            [jnp.concatenate(ahi, axis=0), jnp.concatenate(alo, axis=0)], axis=1
        )
        ampp[...] = dot(lhs, jnp.concatenate([tab[8], tab[8]], axis=0))
        from_left(2, 1)
        from_left(3, 3)
        for which in range(2):
            for r in range(0, half, CH):
                re = ys[2 + which, r : r + CH, :]
                im = ys[2 + which, half + r : half + r + CH, :]
                amp = ampp[which * half + r : which * half + r + CH, :]
                keep = 1.0 - amp * lax.rsqrt(jnp.maximum(re * re + im * im, FLOOR_SQUARE))
                put(which, slice(r, r + CH), all_c, re * keep)
                put(which, slice(half + r, half + r + CH), all_c, im * keep)
        from_left(0, 0)
        from_left(1, 2)
        for r in range(0, half, CH):
            for part, cols in ((0, lo_c), (1, hi_c)):
                even = ys[0, part * half + r : part * half + r + CH, :]
                odd = ys[1, part * half + r : part * half + r + CH, :]
                upper, lower = even + odd, even - odd
                for rows, val in (
                    (slice(r, r + CH), upper), (slice(half + r, half + r + CH), lower),
                ):
                    put(2, rows, cols, val[:, lo_c])
                    put(3, rows, cols, val[:, hi_c])
        from_right(2, 1)
        from_right(3, 3)
        @pl.when(i >= 2)
        def _():
            give(i - 2, buf).wait()

        live = jnp.full((CH, pw), lax.rem(i, MAXL), jnp.int32) < count_ref[lax.div(i, MAXL)]
        for r in range(0, pw, CH):
            rows = slice(r, r + CH)
            even, odd = ys[2, rows, :], ys[3, rows, :]
            plus, minus = even + odd, even - odd
            bre = jnp.concatenate([plus[:, lo_c], minus[:, lo_c]], axis=1)
            bim = jnp.concatenate([plus[:, hi_c], minus[:, hi_c]], axis=1)
            pre = pup[0, rows, pl.ds(pc, pw)].astype(F32)
            pim = pup[1, rows, pl.ds(pc, pw)].astype(F32)
            cre = cbuf[buf, 0, rows, :].astype(F32)
            cim = cbuf[buf, 1, rows, :].astype(F32)
            obuf[buf, 0, rows, :] = pre * bre + pim * bim
            obuf[buf, 1, rows, :] = pre * bim - pim * bre
            pgrad[0, rows, pl.ds(pc, pw)] += jnp.where(live, cre * bre + cim * bim, 0.0)
            pgrad[1, rows, pl.ds(pc, pw)] += jnp.where(live, cre * bim - cim * bre, 0.0)
        give(i, buf).start()
        return 0

    lax.fori_loop(0, total, slot_step, 0)
    for i in range(max(total - 2, 0), total):
        give(i, i % 2).wait()
    for c, ((dy, dx), _, _) in zip(copies, moves):
        @pl.when(has[dy, dx])
        def _(c=c):
            c.wait_send()

        @pl.when(has[-dy, -dx])
        def _(c=c):
            c.wait_recv()


def finish_kernel(
    start_ref, count_ref, flag_ref, spec, pgrad_in, backs_hbm,
    up, down, west, east, pup_up, pup_down, pup_west, pup_east, nw, ne, sw, se,
    out, pgrad,
    acc, stage, backs, rows_buf, sides, hrows, hsides, hcorn, hpv, hph, band_sem, out_sem,
):
    pw = pgrad.shape[1]
    edge = spec.shape[1]
    cols_dev = spec.shape[2] // edge
    band = 2 * H
    win_r, win_c = pw + SUB, pw + LANES
    win_t = win_c // LANES
    last = edge // LANES - 1
    w_top, w_bot, w_left, w_right = (flag_ref[i] for i in range(4))
    loads = [
        (spec.at[:, 0:band, :], rows_buf.at[0]),
        (spec.at[:, edge - band :, :], rows_buf.at[1]),
    ]
    for s in range(cols_dev):
        for j, c0 in enumerate((s * edge, (s + 1) * edge - band)):
            loads.append((spec.at[:, :, c0 : c0 + band], sides.at[2 * s + j]))
    loads += [
        (up, hrows.at[0]), (down, hrows.at[1]), (west, hsides.at[0]), (east, hsides.at[1]),
        (nw, hcorn.at[0]), (ne, hcorn.at[1]), (sw, hcorn.at[2]), (se, hcorn.at[3]),
        (pup_up, hpv.at[0]), (pup_down, hpv.at[1]), (pup_west, hph.at[0]), (pup_east, hph.at[1]),
        (backs_hbm, backs),
    ]
    loads = [
        pltpu.make_async_copy(src, dst, band_sem.at[n]) for n, (src, dst) in enumerate(loads)
    ]
    for c in loads:
        c.start()

    def zero_acc(seg):
        def zero(i, _):
            r = pl.multiple_of(i * 8, 8)
            for p in range(2):
                for t in range(edge // LANES):
                    acc[seg, p, t, pl.ds(r, 8), :] = jnp.zeros((8, LANES), F32)
            return 0

        lax.fori_loop(0, edge // 8, zero, 0)

    def own_terms(seg):
        wl = jnp.where(seg == 0, w_left, 1.0)
        wr = jnp.where(seg == cols_dev - 1, w_right, 1.0)
        il = jnp.where(seg == 0, 0.0, 1.0)
        ir = jnp.where(seg == cols_dev - 1, 0.0, 1.0)
        lo_nb = jnp.maximum(2 * seg - 1, 0)
        hi_nb = jnp.minimum(2 * seg + 2, 2 * cols_dev - 1)
        cbase = pl.multiple_of(seg * edge, LANES)

        def side(i, _):
            r = pl.multiple_of(i * SUB, SUB)
            vert = 1.0 + jnp.where(r < band, w_top, 0.0) + jnp.where(r >= edge - band, w_bot, 0.0)
            for p in range(2):
                mine = sides[2 * seg, p, pl.ds(r, SUB), :].astype(F32)
                other = sides[lo_nb, p, pl.ds(r, SUB), :].astype(F32)
                acc[seg, p, 0, pl.ds(r, SUB), :] += MU_WEIGHT * (wl * vert * mine - il * other)
                mine = sides[2 * seg + 1, p, pl.ds(r, SUB), :].astype(F32)
                other = sides[hi_nb, p, pl.ds(r, SUB), :].astype(F32)
                acc[seg, p, last, pl.ds(r, SUB), :] += MU_WEIGHT * (
                    wr * vert * mine - ir * other
                )
            return 0

        lax.fori_loop(0, edge // SUB, side, 0)

        def flat(i, _):
            r = pl.multiple_of(i * SUB, SUB)
            for p in range(2):
                for j, w in ((0, w_top), (1, w_bot)):
                    mine = rows_buf[j, p, pl.ds(r, SUB), pl.ds(cbase, edge)].astype(F32)
                    rs = pl.ds(pl.multiple_of(r + j * (edge - band), SUB), SUB)
                    for t in range(edge // LANES):
                        acc[seg, p, t, rs, :] += (MU_WEIGHT * w) * mine[
                            :, t * LANES : (t + 1) * LANES
                        ]
            return 0

        lax.fori_loop(0, band // SUB, flat, 0)

    def halo_terms(seg):
        def rows_part(j, edge_row):
            def step(i, _):
                r = pl.multiple_of(i * SUB, SUB)
                rs = pl.ds(pl.multiple_of(r + edge_row, SUB), SUB)
                for p in range(2):
                    cb = pl.multiple_of(seg * edge, LANES)
                    wide = hrows[j, p, pl.ds(r, SUB), pl.ds(cb, edge)].astype(F32)
                    for t in range(last + 1):
                        acc[seg, p, t, rs, :] -= MU_WEIGHT * wide[:, t * LANES : (t + 1) * LANES]
                return 0

            lax.fori_loop(0, band // SUB, step, 0)

            def corner(t, fetch):
                for p in range(2):
                    for r in range(0, band, SUB):
                        rs = slice(edge_row + r, edge_row + r + SUB)
                        acc[seg, p, t, rs, :] -= MU_WEIGHT * fetch(p, slice(r, r + SUB)).astype(F32)

            @pl.when(seg > 0)
            def _():
                c0 = pl.multiple_of(seg * edge - LANES, LANES)
                corner(0, lambda p, r: hrows[j, p, r, pl.ds(c0, LANES)])

            @pl.when(seg < cols_dev - 1)
            def _():
                c0 = pl.multiple_of((seg + 1) * edge, LANES)
                corner(last, lambda p, r: hrows[j, p, r, pl.ds(c0, LANES)])

            @pl.when((seg == 0) & (w_left > 0.0))
            def _():
                corner(0, lambda p, r: hcorn[2 * j, p, r, :])

            @pl.when((seg == cols_dev - 1) & (w_right > 0.0))
            def _():
                corner(last, lambda p, r: hcorn[2 * j + 1, p, r, :])

            pc = pl.multiple_of(seg * pw, LANES)
            for p in range(2):
                for r in range(0, pw, CH):
                    rows = slice(r, r + CH)
                    pgrad[p, rows, pl.ds(pc, pw)] -= LAM_WEIGHT * hpv[
                        j, p, rows, pl.ds(pc, pw)
                    ].astype(F32)

        def cols_part(j, t):
            def step(i, _):
                rs = pl.ds(pl.multiple_of(i * CH, CH), CH)
                for p in range(2):
                    acc[seg, p, t, rs, :] -= MU_WEIGHT * hsides[j, p, rs, :].astype(F32)
                return 0

            lax.fori_loop(0, edge // CH, step, 0)
            pc = pl.multiple_of(seg * pw, LANES)
            for p in range(2):
                for r in range(0, pw, CH):
                    rows = slice(r, r + CH)
                    pgrad[p, rows, pl.ds(pc, pw)] -= LAM_WEIGHT * hph[j, p, rows, :].astype(F32)

        @pl.when(w_top > 0.0)
        def _():
            rows_part(0, 0)

        @pl.when(w_bot > 0.0)
        def _():
            rows_part(1, edge - band)

        @pl.when((seg == 0) & (w_left > 0.0))
        def _():
            cols_part(0, 0)

        @pl.when((seg == cols_dev - 1) & (w_right > 0.0))
        def _():
            cols_part(1, last)

    def slot_step(seg, slot):
        a, b, _, b_al = window_of(start_ref, seg, slot, edge, win_r, win_c)
        b_off = b - b_al
        tile0 = b_al // LANES
        n = seg * MAXL + slot
        for r in range(0, pw, CH):
            rows = slice(r, r + CH)
            blank = jnp.zeros((CH, win_c - pw), F32)
            for p in range(2):
                val = backs[n, p, rows, :]
                wide = pltpu.roll(jnp.concatenate([val, blank], axis=1), b_off, axis=1)
                for t in range(win_t):
                    acc[seg, p, tile0 + t, pl.ds(a + r, CH), :] += wide[
                        :, t * LANES : (t + 1) * LANES
                    ]

    quarter = edge // PIECES

    def put_out(seg, q):
        cb = pl.multiple_of(seg * edge, LANES)
        rows = slice(q * quarter, (q + 1) * quarter)
        return pltpu.make_async_copy(
            stage.at[seg, :, rows, :], out.at[:, rows, pl.ds(cb, edge)], out_sem.at[seg, q]
        )

    for s in range(cols_dev):
        zero_acc(s)
    pgrad[...] = pgrad_in[...]
    own_loads = 2 + 2 * cols_dev
    for c in loads[:own_loads]:
        c.wait()

    def segment(seg, _):
        own_terms(seg)

        @pl.when(seg == 0)
        def _():
            for c in loads[own_loads:]:
                c.wait()

        halo_terms(seg)

        def one(slot, _):
            slot_step(seg, slot)
            return 0

        lax.fori_loop(0, count_ref[seg], one, 0)

        def conv(i, _):
            rs = pl.ds(pl.multiple_of(i * SUB, SUB), SUB)
            for p in range(2):
                for t in range(edge // LANES):
                    stage[seg, p, rs, t * LANES : (t + 1) * LANES] = acc[
                        seg, p, t, rs, :
                    ].astype(BF16)
            return 0

        steps = quarter // SUB
        for q in range(PIECES):
            lax.fori_loop(q * steps, (q + 1) * steps, conv, 0)
            put_out(seg, q).start()
        return 0

    lax.fori_loop(0, cols_dev, segment, 0)
    for s in range(cols_dev):
        for q in range(PIECES):
            put_out(s, q).wait()


def local(spectrum, pupils, amplitudes, crop_starts, led_counts):
    cols_dev = amplitudes.shape[1]
    total = cols_dev * MAXL
    pw = pupils.shape[1]
    edge = spectrum.shape[1]
    width = spectrum.shape[2]
    pwide = pupils.shape[2]
    band = 2 * H
    iy, ix = lax.axis_index("sy"), lax.axis_index("sx")
    flags = jnp.stack(
        [iy > 0, iy < lax.axis_size("sy") - 1, ix > 0, ix < lax.axis_size("sx") - 1]
    ).astype(F32)
    table = jnp.asarray(half_tables(pw))
    smem = pl.BlockSpec(memory_space=pltpu.SMEM)
    vmem = pl.BlockSpec(memory_space=pltpu.VMEM)
    hbm = pl.BlockSpec(memory_space=pltpu.HBM)
    win_r, win_c = pw + SUB, pw + LANES
    starts = crop_starts.reshape(-1)
    counts = led_counts.reshape(-1)
    sds = jax.ShapeDtypeStruct
    crops = pl.pallas_call(
        crop_kernel,
        out_shape=sds((total, 2, pw, pw), BF16),
        in_specs=[smem, smem, hbm],
        out_specs=vmem,
        scratch_shapes=[
            pltpu.VMEM((2, 2, win_r, win_c), BF16),
            pltpu.VMEM((2, win_c // LANES, win_r, LANES), F32),
            pltpu.SemaphoreType.DMA((2,)),
        ],
        compiler_params=pltpu.CompilerParams(vmem_limit_bytes=GRANT),
        name="crops",
    )(starts, counts, spectrum)
    rows_s, cols_s = sds((2, band, width), BF16), sds((2, edge, band), BF16)
    pv_s, ph_s, corner_s = sds(pupils.shape, BF16), sds((2, pw, pw), BF16), sds((2, band, band), BF16)
    halos = (rows_s, rows_s, cols_s, cols_s, pv_s, pv_s, ph_s, ph_s) + (corner_s,) * 4
    pgrad, backs, *around = pl.pallas_call(
        wave_kernel,
        out_shape=(sds(pupils.shape, F32), sds((total, 2, pw, pw), F32)) + halos,
        in_specs=[smem, smem, hbm, hbm, hbm, hbm, vmem, vmem],
        out_specs=(vmem, hbm) + (hbm,) * len(halos),
        scratch_shapes=[
            pltpu.VMEM((2, pw // LANES, pw, LANES), F32),
            pltpu.VMEM((2, 2, pw, pw), BF16),
            pltpu.VMEM((2, 2, pw, pw), F32),
            pltpu.VMEM((4, 2, pw, pw), BF16),
            pltpu.VMEM((4, pw, pw), F32),
            pltpu.VMEM((pw, pw), F32),
            pltpu.SemaphoreType.DMA((1 + pw // LANES, 2)),
            pltpu.SemaphoreType.DMA((2,)),
            pltpu.SemaphoreType.DMA((len(halos),)),
            pltpu.SemaphoreType.DMA((len(halos),)),
        ],
        compiler_params=pltpu.CompilerParams(
            vmem_limit_bytes=GRANT, collective_id=0, has_side_effects=True
        ),
        name="waves",
    )(counts, flags, spectrum, pupils, amplitudes[0], crops, pupils, table)
    return pl.pallas_call(
        finish_kernel,
        out_shape=(sds(spectrum.shape, BF16), sds(pupils.shape, F32)),
        in_specs=[smem, smem, smem, hbm, vmem, hbm] + [hbm] * len(halos),
        out_specs=(hbm, vmem),
        scratch_shapes=[
            pltpu.VMEM((cols_dev, 2, edge // LANES, edge, LANES), F32),
            pltpu.VMEM((cols_dev, 2, edge, edge), BF16),
            pltpu.VMEM((total, 2, pw, pw), F32),
            pltpu.VMEM((2, 2, band, width), BF16),
            pltpu.VMEM((2 * cols_dev, 2, edge, band), BF16),
            pltpu.VMEM((2,) + rows_s.shape, BF16),
            pltpu.VMEM((2,) + cols_s.shape, BF16),
            pltpu.VMEM((4,) + corner_s.shape, BF16),
            pltpu.VMEM((2,) + pv_s.shape, BF16),
            pltpu.VMEM((2,) + ph_s.shape, BF16),
            pltpu.SemaphoreType.DMA((3 + 2 * cols_dev + len(halos),)),
            pltpu.SemaphoreType.DMA((cols_dev, PIECES)),
        ],
        compiler_params=pltpu.CompilerParams(vmem_limit_bytes=GRANT),
        name="finish",
    )(starts, counts, flags, spectrum, pgrad, backs, *around)


def solution(mesh):
    placed = (
        P(None, "sy", "sx"),
        P(None, "sy", "sx"),
        P("sy", "sx", None, None, None),
        P("sy", "sx", None, None),
        P("sy", "sx"),
    )
    return jax.shard_map(
        local,
        mesh=mesh,
        in_specs=placed,
        out_specs=(P(None, "sy", "sx"), P(None, "sy", "sx")),
        check_vma=False,
    )
```
